32 devices in a mesh: tp: 4 (over z), dp: 2 (over y), pp: 4 (over x, core).
Axes of the slice: x: 2, y: 2, z: 4, core: 2. Of those that a mesh axis runs over, the one named last changes fastest.
Arguments:
- master: float32 [50304, 768], P('tp')
- exp_avg: float32 [50304, 768], P('tp')
- exp_avg_sq: float32 [50304, 768], P('tp')
- stage_ids: int32 [4, 16, 384], P('pp', 'dp')
- stage_acts: bfloat16 [4, 16, 384, 768], P('pp', 'dp')
Outputs:
- output 1: float32 [50304, 768], P('tp')
- output 2: float32 [50304, 768], P('tp')
- output 3: float32 [50304, 768], P('tp')
- output 4: bfloat16 [50304, 768], P('tp')
All inputs are finite; a program needn't handle non-finite values.
Results may differ from the reference program's by a relative error of at most 0.001.
Values sent between devices are 32-bit elements.
A program may use at most 1 GiB of HBM per device.

```python
import math
import jax
import jax.numpy as jnp
from jax import lax

VOCAB_SIZE = 50304
MODEL_DIM = 768
SEQ_LEN = 384
BATCH_DEV = 8
DATA_REPL = 2
PIPE_STAGES = 4
OPT_STEP = 10
TOKEN_BLOCK = 128

BATCH_ALL = BATCH_DEV * DATA_REPL
TOKENS_REPL = BATCH_DEV * SEQ_LEN
LOG_SPAN = math.ceil(math.log2(VOCAB_SIZE))
LEARN_RATE = 0.003
BETA_ONE = 0.9
BETA_TWO = 0.95
ADAM_EPS = 1e-8
WEIGHT_DECAY = 0.1
CLIP_NORM = 1.0


def draw_ids(key, perm):
    key_exp, key_rank = jax.random.split(key)
    ids_shape = (PIPE_STAGES, BATCH_ALL, SEQ_LEN)
    exponents = jax.random.randint(key_exp, ids_shape, 0, LOG_SPAN + 1)
    upper_bound = jnp.minimum(jnp.left_shift(jnp.int32(1), exponents), VOCAB_SIZE)
    ranks = jax.random.randint(key_rank, ids_shape, 0, upper_bound)
    tokens = perm[ranks]
    tokens = tokens.at[:, 0, 0].set(0)
    tokens = tokens.at[:, BATCH_ALL - 1, SEQ_LEN - 1].set(VOCAB_SIZE - 1)
    return tokens.astype(jnp.int32)


def setup_inputs(seed: int = 0) -> dict:
    key = jax.random.key(seed)
    k_tab, k_avg, k_sq, k_perm, k_ids, k_act, k_hid = jax.random.split(key, 7)
    table_shape = (VOCAB_SIZE, MODEL_DIM)
    elem_scale = (VOCAB_SIZE * MODEL_DIM) ** -0.5
    master = jax.random.normal(k_tab, table_shape, jnp.float32) * MODEL_DIM ** -0.5
    exp_avg = jax.random.normal(k_avg, table_shape, jnp.float32) * (0.3 * elem_scale)
    exp_avg_sq = jnp.exp(0.5 * jax.random.normal(k_sq, table_shape, jnp.float32)) * (0.09 * elem_scale * elem_scale)
    perm = jax.random.permutation(k_perm, VOCAB_SIZE)
    stage_ids = draw_ids(k_ids, perm)
    grad_scale = 0.08 * math.sqrt(DATA_REPL / TOKENS_REPL)
    stage_acts = jax.random.normal(k_act, (PIPE_STAGES, BATCH_ALL, SEQ_LEN, MODEL_DIM), jnp.float32) * grad_scale
    label_pull = math.log(VOCAB_SIZE) / math.sqrt(MODEL_DIM)
    noise = jax.random.normal(k_hid, (BATCH_ALL, SEQ_LEN, MODEL_DIM), jnp.float32)
    hidden = math.sqrt(1.0 - label_pull * label_pull) * noise + (label_pull * math.sqrt(MODEL_DIM)) * master[stage_ids[PIPE_STAGES - 1]]
    stage_acts = stage_acts.at[PIPE_STAGES - 1].set(hidden)
    return {"master": master, "exp_avg": exp_avg, "exp_avg_sq": exp_avg_sq, "stage_ids": stage_ids, "stage_acts": stage_acts.astype(jnp.bfloat16)}


def head_block(table_bf, hid_block, lab_block):
    logits = jnp.dot(hid_block, table_bf.T, preferred_element_type=jnp.float32)
    prob_mat = jax.nn.softmax(logits, axis=-1)
    is_label = lab_block[:, None] == jnp.arange(VOCAB_SIZE, dtype=jnp.int32)[None, :]
    dlogits = (jnp.where(is_label, prob_mat - 1.0, prob_mat) / TOKENS_REPL).astype(jnp.bfloat16)
    return jnp.dot(dlogits.T, hid_block, preferred_element_type=jnp.float32)


def replica_grad(table_bf, ids_in, dx_in, hidden, labels):
    grad_embed = jax.ops.segment_sum(dx_in.astype(jnp.float32), ids_in, num_segments=VOCAB_SIZE)

    def add_block(acc_grad, block_in):
        return acc_grad + head_block(table_bf, block_in[0], block_in[1]), None

    hid_blocks = hidden.reshape(-1, TOKEN_BLOCK, MODEL_DIM)
    lab_blocks = labels.reshape(-1, TOKEN_BLOCK)
    return lax.scan(add_block, grad_embed, (hid_blocks, lab_blocks))[0]


def reference(master, exp_avg, exp_avg_sq, stage_ids, stage_acts):
    table_bf = master.astype(jnp.bfloat16)
    ids_in = stage_ids[0].reshape(DATA_REPL, TOKENS_REPL)
    labels = stage_ids[PIPE_STAGES - 1].reshape(DATA_REPL, TOKENS_REPL)
    dx_in = stage_acts[0].reshape(DATA_REPL, TOKENS_REPL, MODEL_DIM)
    hidden = stage_acts[PIPE_STAGES - 1].reshape(DATA_REPL, TOKENS_REPL, MODEL_DIM)

    def add_replica(acc_grad, block_in):
        return acc_grad + replica_grad(table_bf, block_in[0], block_in[1], block_in[2], block_in[3]), None

    zero_grad = jnp.zeros((VOCAB_SIZE, MODEL_DIM), jnp.float32)
    grad_sum = lax.scan(add_replica, zero_grad, (ids_in, dx_in, hidden, labels))[0]
    gradient = grad_sum / DATA_REPL
    norm_val = jnp.sqrt(jnp.sum(gradient * gradient))
    gradient = gradient * (CLIP_NORM / jnp.maximum(norm_val, CLIP_NORM))
    new_avg = BETA_ONE * exp_avg + (1.0 - BETA_ONE) * gradient
    new_avg_sq = BETA_TWO * exp_avg_sq + (1.0 - BETA_TWO) * gradient * gradient
    corr_one = 1.0 - BETA_ONE ** OPT_STEP
    corr_two = 1.0 - BETA_TWO ** OPT_STEP
    step_dir = (new_avg / corr_one) / (jnp.sqrt(new_avg_sq / corr_two) + ADAM_EPS)
    new_master = master - LEARN_RATE * (step_dir + WEIGHT_DECAY * master)
    return new_master, new_avg, new_avg_sq, new_master.astype(jnp.bfloat16)
```

```python
import functools

import jax
import jax.numpy as jnp
from jax import lax
from jax.experimental import pallas as pl
from jax.experimental.pallas import tpu as pltpu
from jax.sharding import PartitionSpec as P

LEARN_RATE = 0.003
BETA_ONE = 0.9
BETA_TWO = 0.95
ADAM_EPS = 1e-8
WEIGHT_DECAY = 0.1
CLIP_NORM = 1.0
OPT_STEP = 10

ROW_STEP = 264
TOK_STEP = 512
ADAMW_FLOPS = 2000
VMEM_LIMIT = 60 * 1024 * 1024


def dot_nt(a, b):
    return lax.dot_general(a, b, (((1,), (1,)), ((), ())), preferred_element_type=jnp.float32)


SPREAD_CHUNKS = 16
MESH = pl.DeviceIdType.MESH


def spread_kernel(act_ref, ids_ref, hid_ref, look_ref, all_ids_ref, buf, ids_buf, sx, sy, sz, sd, sl, si, load, recv, recv_core, recv_ids):
    z, y, p = lax.axis_index("tp"), lax.axis_index("dp"), lax.axis_index("pp")
    x, core, odd = p // 2, p % 2, z % 2
    x_dev = {"pp": (1 - x) * 2 + core}
    y_dev = {"dp": 1 - y}
    z_dev = {"tp": z + 1 - 2 * odd}
    core_dev = {"pp": x * 2 + 1 - core}
    plane = [{"dp": (y + dy) % 2, "pp": (p + dp) % 4} for dy in range(2) for dp in range(4) if dy + dp > 0]
    n = SPREAD_CHUNKS
    edge, main = n // 4, 3 * n // 4
    tok = act_ref.shape[0]
    size = tok // n

    barrier = pltpu.get_barrier_semaphore()
    for dev in plane + [z_dev]:
        pl.semaphore_signal(barrier, inc=1, device_id=dev, device_id_type=MESH)
    pl.semaphore_wait(barrier, len(plane) + 1)

    def chunk(i):
        if i < edge:
            return odd * main + i
        return i if i < main else (1 - odd) * main + (i - main)

    def span(replica, i):
        return pl.ds(pl.multiple_of(replica * tok + chunk(i) * size, size), size)

    def remote(src, dst, send_sem, recv_sem, dev):
        copy = pltpu.make_async_remote_copy(src_ref=src, dst_ref=dst, send_sem=send_sem, recv_sem=recv_sem, device_id=dev, device_id_type=MESH)
        copy.start()
        return copy

    def send_ids(kind):
        local = pltpu.make_async_copy(ids_ref, ids_buf.at[kind, y], recv_ids.at[kind, y])
        local.start()
        for i, dev in enumerate(plane):
            remote(ids_ref, ids_buf.at[kind, y], si.at[i], recv_ids.at[kind, y], dev)

    def drain_ids():
        for i in range(len(plane)):
            pltpu.make_async_copy(ids_ref, ids_ref, si.at[i]).wait()

    pl.when(p == 0)(lambda: send_ids(0))
    pl.when(p == 3)(lambda: send_ids(1))

    def run(out_ref, x_src):

        def send(replica, i, send_sem, recv_sem, dev):
            view = buf.at[span(replica, i)]
            return remote(view, view, send_sem, recv_sem, dev)

        def arrived(replica, i, slot):
            view = buf.at[span(replica, i)]
            pltpu.make_async_copy(view, view, recv.at[slot, i]).wait()

        def keep(copies, replica, i, slot):
            view, place = buf.at[span(replica, i)], out_ref.at[span(replica, i)]
            copies.append(remote(view, place, sd.at[slot, i], recv_core.at[slot, i], core_dev).wait_send)
            local = pltpu.make_async_copy(view, place, sl.at[slot, i])
            local.start()
            copies.append(local.wait)

        @pl.when(x == x_src)
        def _():
            copies, loads = [], []
            for i in range(n):
                rows = pl.ds(pl.multiple_of(chunk(i) * size, size), size)
                loads.append(pltpu.make_async_copy(act_ref.at[rows], buf.at[span(y, i)], load.at[i]))
                loads[-1].start()
            for i in range(n):
                loads[i].wait()
                if i < edge:
                    copies.append(send(y, i, sx.at[i], recv.at[0, i], x_dev).wait_send)
                if i < main:
                    copies.append(send(y, i, sy.at[i], recv.at[1, i], y_dev).wait_send)
            for i in range(n):
                keep(copies, y, i, 0)
            for i in range(main):
                arrived(1 - y, i, 1)
                if i + edge < main:
                    copies.append(send(y, i + edge, sx.at[i + edge], recv.at[0, i + edge], x_dev).wait_send)
                if i % 2 == 0:
                    copies.append(send(1 - y, i, sx.at[main + i // 2], recv.at[1, i], x_dev).wait_send)
                if i < edge:
                    copies.append(send(1 - y, i, sz.at[1, i], recv.at[1, main + i], z_dev).wait_send)
                keep(copies, 1 - y, i, 1)
            for i in range(main, n):
                arrived(1 - y, i, 1)
                keep(copies, 1 - y, i, 1)
            for wait in copies:
                wait()

        @pl.when(x != x_src)
        def _():
            copies = []
            for s in range(main + edge):
                if s < main:
                    arrived(y, s, 0)
                    if s % 2 == 1:
                        copies.append(send(y, s, sy.at[s], recv.at[1, s], y_dev).wait_send)
                    if s < edge:
                        copies.append(send(y, s, sz.at[0, s], recv.at[0, main + s], z_dev).wait_send)
                    keep(copies, y, s, 0)
                if s >= edge:
                    i = s - edge
                    arrived(1 - y, i, 1)
                    if i < edge:
                        copies.append(send(1 - y, i, sz.at[1, i], recv.at[1, main + i], z_dev).wait_send)
                    keep(copies, 1 - y, i, 1)
            for i in range(main, n):
                for slot, replica in ((0, y), (1, 1 - y)):
                    arrived(replica, i, slot)
                    keep(copies, replica, i, slot)
            for wait in copies:
                wait()

    def wait_core(out_ref):
        for slot, replica in ((0, y), (1, 1 - y)):
            for i in range(n):
                view = out_ref.at[span(replica, i)]
                pltpu.make_async_copy(view, view, recv_core.at[slot, i]).wait()

    @pl.when(core == 1)
    def _():
        run(hid_ref, 1)
        wait_core(look_ref)

    @pl.when(core == 0)
    def _():
        run(look_ref, 0)
        wait_core(hid_ref)

    for kind in range(2):
        for replica in range(2):
            pltpu.make_async_copy(ids_ref, ids_buf.at[kind, replica], recv_ids.at[kind, replica]).wait()
    pl.when(p == 0)(drain_ids)
    pl.when(p == 3)(drain_ids)
    all_ids_ref[...] = ids_buf[...]


def spread_call(acts, ids, n_repl):
    tok, dim = acts.shape
    n = SPREAD_CHUNKS
    shape = jax.ShapeDtypeStruct((n_repl * tok, dim), jnp.float32)
    ids_shape = (2, n_repl) + ids.shape
    dma = pltpu.SemaphoreType.DMA
    return pl.pallas_call(
        spread_kernel,
        in_specs=[pl.BlockSpec(memory_space=pl.ANY), pl.BlockSpec(memory_space=pltpu.VMEM)],
        out_specs=[pl.BlockSpec(memory_space=pl.ANY)] * 2 + [pl.BlockSpec(memory_space=pltpu.VMEM)],
        out_shape=[shape, shape, jax.ShapeDtypeStruct(ids_shape, jnp.int32)],
        scratch_shapes=[
            pltpu.VMEM((n_repl * tok, dim), jnp.float32), pltpu.VMEM(ids_shape, jnp.int32),
            dma((n + n // 2,)), dma((n,)), dma((2, n // 4)), dma((2, n)), dma((2, n)), dma((8,)),
            dma((n,)), dma((2, n)), dma((2, n)), dma((2, 2)),
        ],
        compiler_params=pltpu.CompilerParams(collective_id=0, has_side_effects=True, vmem_limit_bytes=VMEM_LIMIT),
        name="spread",
    )(acts, ids)


def slice_partners(z, y, p):
    return [
        {"pp": (p // 2) * 2 + 1 - p % 2}, {"pp": (1 - p // 2) * 2 + p % 2}, {"dp": 1 - y},
        {"tp": z + 1 - 2 * (z % 2)}, {"tp": (z + 2) % 4},
    ]


def meet(partners):
    barrier = pltpu.get_barrier_semaphore()
    for dev in partners:
        pl.semaphore_signal(barrier, inc=1, device_id=dev, device_id_type=MESH)
    pl.semaphore_wait(barrier, len(partners))


def combine_kernel(scale, in_ref, top_ref, inv_ref, mine, theirs, send_sem, recv_sem):
    z, y, p = lax.axis_index("tp"), lax.axis_index("dp"), lax.axis_index("pp")
    partners = slice_partners(z, y, p)
    meet(partners)
    half = in_ref.shape[0] // 2
    mine[0] = in_ref[...]
    for step, dev in enumerate(partners):
        copy = pltpu.make_async_remote_copy(src_ref=mine.at[step], dst_ref=theirs.at[step], send_sem=send_sem.at[step], recv_sem=recv_sem.at[step], device_id=dev, device_id_type=MESH)
        copy.start()
        copy.wait()
        top_a, sum_a = mine[step, :half], mine[step, half:]
        top_b, sum_b = theirs[step, :half], theirs[step, half:]
        top = jnp.maximum(top_a, top_b)
        total = sum_a * jnp.exp(top_a - top) + sum_b * jnp.exp(top_b - top)
        if step + 1 < len(partners):
            mine[step + 1, :half] = top
            mine[step + 1, half:] = total
        else:
            top_ref[...] = top
            inv_ref[...] = 1.0 / (total * scale)


def combine_call(local, scale):
    rows, lanes = local.shape
    shape = jax.ShapeDtypeStruct((rows // 2, lanes), jnp.float32)
    return pl.pallas_call(
        functools.partial(combine_kernel, scale),
        in_specs=[pl.BlockSpec(memory_space=pltpu.VMEM)],
        out_specs=[pl.BlockSpec(memory_space=pltpu.VMEM)] * 2,
        out_shape=[shape, shape],
        scratch_shapes=[pltpu.VMEM((5, rows, lanes), jnp.float32), pltpu.VMEM((5, rows, lanes), jnp.float32), pltpu.SemaphoreType.DMA((5,)), pltpu.SemaphoreType.DMA((5,))],
        compiler_params=pltpu.CompilerParams(collective_id=1, has_side_effects=True),
        name="combine",
    )(local)


def stats_kernel(scal_ref, table_ref, act_ref, max_ref, sum_ref, cast_ref):
    act = act_ref[...].astype(jnp.bfloat16)
    cast_ref[...] = act
    rows = table_ref.shape[0]
    parts = []
    for start in range(0, rows, ROW_STEP):
        logits = dot_nt(table_ref[start:start + ROW_STEP, :], act)
        if start + ROW_STEP == rows:
            row = start + lax.broadcasted_iota(jnp.int32, logits.shape, 0)
            logits = jnp.where(row < scal_ref[1], logits, -jnp.inf)
        top = jnp.max(logits, axis=0, keepdims=True)
        parts.append((top, jnp.sum(jnp.exp(logits - top), axis=0, keepdims=True)))
    top_all = functools.reduce(jnp.maximum, [p[0] for p in parts])
    max_ref[...] = top_all
    sum_ref[...] = functools.reduce(jnp.add, [p[1] * jnp.exp(p[0] - top_all) for p in parts])


def stats_call(scal, table_bf, acts):
    tokens, dim = acts.shape
    rows = table_bf.shape[0]
    return pl.pallas_call(
        stats_kernel,
        grid=(tokens // TOK_STEP,),
        in_specs=[
            pl.BlockSpec(memory_space=pltpu.SMEM),
            pl.BlockSpec((rows, dim), lambda t: (0, 0)),
            pl.BlockSpec((TOK_STEP, dim), lambda t: (t, 0)),
        ],
        out_specs=[
            pl.BlockSpec((1, TOK_STEP), lambda t: (0, t)),
            pl.BlockSpec((1, TOK_STEP), lambda t: (0, t)),
            pl.BlockSpec((TOK_STEP, dim), lambda t: (t, 0)),
        ],
        out_shape=[
            jax.ShapeDtypeStruct((1, tokens), jnp.float32),
            jax.ShapeDtypeStruct((1, tokens), jnp.float32),
            jax.ShapeDtypeStruct((tokens, dim), jnp.bfloat16),
        ],
        compiler_params=pltpu.CompilerParams(vmem_limit_bytes=VMEM_LIMIT),
        cost_estimate=pl.CostEstimate(flops=2 * tokens * rows * dim, bytes_accessed=6 * tokens * dim, transcendentals=tokens * rows),
        name="stats",
    )(scal, table_bf, acts)


def norm_kernel(*refs):
    *in_refs, out_ref, mine, theirs, send_sem, recv_sem = refs
    z, y, p = lax.axis_index("tp"), lax.axis_index("dp"), lax.axis_index("pp")
    partners = slice_partners(z, y, p)
    meet(partners)
    total = jnp.full(out_ref.shape, jnp.sum(sum(ref[...] for ref in in_refs)))
    for step, dev in enumerate(partners):
        mine[step] = total
        copy = pltpu.make_async_remote_copy(src_ref=mine.at[step], dst_ref=theirs.at[step], send_sem=send_sem.at[step], recv_sem=recv_sem.at[step], device_id=dev, device_id_type=MESH)
        copy.start()
        copy.wait()
        total = total + theirs[step]
    out_ref[...] = CLIP_NORM / jnp.maximum(jnp.sqrt(total), CLIP_NORM)


def norm_call(squares):
    vmem = pl.BlockSpec(memory_space=pltpu.VMEM)
    return pl.pallas_call(
        norm_kernel,
        in_specs=[vmem] * len(squares),
        out_specs=vmem,
        out_shape=jax.ShapeDtypeStruct((8, 128), jnp.float32),
        scratch_shapes=[pltpu.VMEM((5, 8, 128), jnp.float32), pltpu.VMEM((5, 8, 128), jnp.float32), pltpu.SemaphoreType.DMA((5,)), pltpu.SemaphoreType.DMA((5,))],
        compiler_params=pltpu.CompilerParams(collective_id=2, has_side_effects=True),
        name="norm",
    )(*squares)


def grad_kernel(offset, tok_count, scal_ref, table_ref, hid_ref, dx_ref, max_ref, inv_ref, lab_ref, ids_ref, *out_refs):
    *grad_refs, sq_ref = out_refs
    step = pl.program_id(0)
    rows = grad_refs[0].shape[0]

    @pl.when(step == 0)
    def _():
        for grad_ref in grad_refs:
            grad_ref[...] = jnp.zeros_like(grad_ref)

    hid = hid_ref[...]
    look = dx_ref[...].astype(jnp.bfloat16)
    for start in range(0, rows * len(grad_refs), ROW_STEP):
        logits = dot_nt(table_ref[start:start + ROW_STEP, :], hid)
        local = offset + start + lax.broadcasted_iota(jnp.int32, logits.shape, 0)
        row = jnp.where(local < scal_ref[1], local + scal_ref[0], -1)
        prob = jnp.where(local < scal_ref[1], jnp.exp(logits - max_ref[...]) * inv_ref[...], 0.0)
        dlog = (prob - jnp.where(row == lab_ref[...], 1.0 / tok_count, 0.0)).astype(jnp.bfloat16)
        hot = jnp.where(row == ids_ref[...], 1.0, 0.0).astype(jnp.bfloat16)
        part = jnp.dot(dlog, hid, preferred_element_type=jnp.float32)
        part += jnp.dot(hot, look, preferred_element_type=jnp.float32)
        grad_refs[start // rows][start % rows:start % rows + ROW_STEP, :] += part

    @pl.when(step == pl.num_programs(0) - 1)
    def _():
        square = jnp.zeros_like(sq_ref)
        for grad_ref in grad_refs:
            grad = grad_ref[...] * 0.5
            grad_ref[...] = grad
            square += jnp.sum(grad * grad, axis=0, keepdims=True)
        sq_ref[...] = square


def grad_call(scal, table_bf, hid, dx, top, inv, labels, ids, offset, rows, n_out, tok_count):
    tokens, dim = hid.shape
    tok_spec = pl.BlockSpec((1, TOK_STEP), lambda t: (0, t))
    act_spec = pl.BlockSpec((TOK_STEP, dim), lambda t: (t, 0))
    return pl.pallas_call(
        functools.partial(grad_kernel, offset, tok_count),
        grid=(tokens // TOK_STEP,),
        in_specs=[
            pl.BlockSpec(memory_space=pltpu.SMEM),
            pl.BlockSpec((rows * n_out, dim), lambda t: (0, 0)),
            act_spec, act_spec, tok_spec, tok_spec, tok_spec, tok_spec,
        ],
        out_specs=[pl.BlockSpec((rows, dim), lambda t: (0, 0))] * n_out + [pl.BlockSpec((1, dim), lambda t: (0, 0))],
        out_shape=[jax.ShapeDtypeStruct((rows, dim), jnp.float32)] * n_out + [jax.ShapeDtypeStruct((1, dim), jnp.float32)],
        compiler_params=pltpu.CompilerParams(vmem_limit_bytes=VMEM_LIMIT),
        cost_estimate=pl.CostEstimate(flops=6 * tokens * rows * n_out * dim, bytes_accessed=6 * tokens * dim, transcendentals=tokens * rows * n_out),
        name=f"grad_{offset}",
    )(scal, table_bf[offset:offset + rows * n_out], hid, dx, top, inv, labels, ids)


def adamw_kernel(groups, n_alias, *refs):
    n_piece = sum(groups)
    scale_ref, master_ref, avg_ref, sq_ref = refs[1:5]
    piece_refs = refs[5:5 + n_piece]
    out_master, out_avg, out_sq, out_bf, out_scale = refs[5 + n_piece + n_alias:]
    out_scale[...] = scale_ref[...]
    step = pl.program_id(0)
    scale = scale_ref[0:1, 0:1]
    sub_rows = 88

    def update(grad_ref, base):
        def body(i, carry):
            start = pl.multiple_of(i * sub_rows, 8)
            rows = pl.ds(base + start, sub_rows)
            grad = grad_ref[pl.ds(start, sub_rows), :] * scale
            avg = BETA_ONE * avg_ref[rows, :] + (1.0 - BETA_ONE) * grad
            sq = BETA_TWO * sq_ref[rows, :] + (1.0 - BETA_TWO) * grad * grad
            step_dir = (avg / (1.0 - BETA_ONE ** OPT_STEP)) / (jnp.sqrt(sq / (1.0 - BETA_TWO ** OPT_STEP)) + ADAM_EPS)
            old = master_ref[rows, :]
            new = old - LEARN_RATE * (step_dir + WEIGHT_DECAY * old)
            out_master[rows, :] = new
            out_avg[rows, :] = avg
            out_sq[rows, :] = sq
            out_bf[rows, :] = new.astype(jnp.bfloat16)
            return carry

        lax.fori_loop(0, grad_ref.shape[0] // sub_rows, body, 0)

    def update_group(group):
        base = 0
        for ref in group:
            update(ref, base)
            base += ref.shape[0]

    first = 0
    for index, count in enumerate(groups):
        pl.when(step == index)(functools.partial(update_group, piece_refs[first:first + count]))
        first += count


def adamw_call(where, scale, state, groups, outs, name):
    vocab, dim = state[0].shape
    rows = 2 * ROW_STEP
    pieces = [p for group in groups for p in group]
    table_spec = pl.BlockSpec((rows, dim), lambda s, where: (where[s], 0))
    specs = [pl.BlockSpec(p.shape, lambda s, where: (0, 0), pipeline_mode=pl.Buffered(1)) for p in pieces]
    extra = list(outs) if outs is not None else []
    scale_spec = pl.BlockSpec((8, 128), lambda s, where: (0, 0))
    n_in = 2 + 3 + len(pieces)
    shapes = [jax.ShapeDtypeStruct((vocab, dim), jnp.float32)] * 3 + [jax.ShapeDtypeStruct((vocab, dim), jnp.bfloat16)]
    n_el = len(groups) * rows * dim
    return pl.pallas_call(
        functools.partial(adamw_kernel, tuple(len(g) for g in groups), len(extra)),
        grid_spec=pltpu.PrefetchScalarGridSpec(
            num_scalar_prefetch=1,
            grid=(len(groups),),
            in_specs=[scale_spec] + [table_spec] * 3 + specs + [pl.BlockSpec(memory_space=pl.ANY)] * len(extra),
            out_specs=[table_spec] * 4 + [scale_spec],
        ),
        out_shape=shapes + [jax.ShapeDtypeStruct((8, 128), jnp.float32)],
        input_output_aliases={n_in + i: i for i in range(len(extra))},
        compiler_params=pltpu.CompilerParams(vmem_limit_bytes=VMEM_LIMIT),
        cost_estimate=pl.CostEstimate(flops=ADAMW_FLOPS * n_el, bytes_accessed=30 * n_el, transcendentals=n_el),
        name=name,
    )(where, scale, *state, *pieces, *extra)


def solution(mesh):
    n_stage, n_repl = mesh.shape["pp"], mesh.shape["dp"]
    n_plane = n_stage * n_repl
    table_spec = P("tp", None)
    axes = ("tp", "dp", "pp")
    x_swap = [(i, i ^ 2) for i in range(n_stage)]
    core_swap = [(i, i ^ 1) for i in range(n_stage)]
    y_swap = [(0, 1), (1, 0)]

    def device_step(master, exp_avg, exp_avg_sq, stage_ids, stage_acts):
        z, y, p = (lax.axis_index(a) for a in axes)
        vocab, dim = master.shape
        tok = stage_ids.shape[1] * stage_ids.shape[2]
        own_rows = -(-vocab // (n_plane * 6 * ROW_STEP)) * 6 * ROW_STEP
        plane = y * n_stage + p

        first_row = plane * own_rows
        valid = jnp.minimum(own_rows, vocab - first_row)
        short = own_rows * n_plane - vocab
        near = lax.dynamic_slice(master, (jnp.minimum(first_row, vocab - own_rows), 0), (own_rows, dim)).astype(jnp.bfloat16)
        near = jnp.concatenate([near, jnp.zeros((short, dim), jnp.bfloat16)], axis=0)
        table_bf = lax.dynamic_slice(near, (own_rows - valid, 0), (own_rows, dim))
        scal = jnp.stack([z * vocab + first_row, valid]).astype(jnp.int32)

        acts = stage_acts.reshape(tok, dim).astype(jnp.float32)
        hid, dx, all_ids = spread_call(acts, stage_ids.reshape(tok // 128, 128), n_repl)
        ids, labels = all_ids[0].reshape(1, -1), all_ids[1].reshape(1, -1)
        top_own, sum_own, hid_bf = stats_call(scal, table_bf, hid)
        local = jnp.concatenate([top_own.reshape(-1, 128), sum_own.reshape(-1, 128)], axis=0)
        top, inv = (a.reshape(1, -1) for a in combine_call(local, float(tok)))

        rows = 2 * ROW_STEP
        n_chunk = own_rows // rows
        first, sq_first = grad_call(scal, table_bf, hid_bf, dx, top, inv, labels, ids, 0, rows, 1, tok)
        *rest, sq_rest = grad_call(scal, table_bf, hid_bf, dx, top, inv, labels, ids, rows, rows, n_chunk - 1, tok)
        scale = norm_call([sq_first, sq_rest])
        rest, scale = lax.optimization_barrier((rest, scale))
        grads = [first] + list(rest)

        def across(a):
            return lax.ppermute(a, "pp", core_swap)

        def block(c, flip_y, flip_x):
            return lambda q: ((1 - y if flip_y else y) * n_stage + (q ^ 2 if flip_x else q)) * n_chunk + c

        def call(groups, outs, scale, name):
            where = jnp.stack([spot(q) for q in (p, p ^ 1) for _, _, spot in groups])
            arrays = [mine for mine, _, _ in groups] + [theirs for _, theirs, _ in groups]
            *outs, scale = adamw_call(where.astype(jnp.int32), scale, (master, exp_avg, exp_avg_sq), arrays, outs, name)
            return outs, scale

        def corner_of(from_x, from_y):
            return [lax.ppermute(from_x[:ROW_STEP], "dp", y_swap), lax.ppermute(from_y[ROW_STEP:], "pp", x_swap)]

        def direct_group(c, from_x, from_y):
            return [([from_x], [across(from_x)], block(c, False, True)), ([from_y], [across(from_y)], block(c, True, False))]

        def corner_group(c, corner):
            return [(corner, [across(a) for a in corner], block(c, True, True))]

        sent = [(lax.ppermute(g, "pp", x_swap), lax.ppermute(g, "dp", y_swap)) for g in grads]
        corner = corner_of(*sent[0])
        outs, scale = call([([g], [across(g)], block(c, False, False)) for c, g in enumerate(grads)], None, scale, "adamw_own")
        outs, scale = call(direct_group(0, *sent[0]) + corner_group(0, corner), outs, scale, "adamw_0")
        late = []
        for c in range(1, n_chunk):
            (from_x, from_y), scale = lax.optimization_barrier((sent[c], scale))
            late.append(corner_of(from_x, from_y))
            outs, scale = call(direct_group(c, from_x, from_y), outs, scale, f"adamw_{c}")
        for c in range(1, n_chunk):
            corner, scale = lax.optimization_barrier((late[c - 1], scale))
            outs, scale = call(corner_group(c, corner), outs, scale, f"corner_{c}")
        return tuple(outs)

    return jax.shard_map(device_step, mesh=mesh, in_specs=(table_spec, table_spec, table_spec, P("pp", "dp", None), P("pp", "dp", None, None)), out_specs=(table_spec, table_spec, table_spec, table_spec), check_vma=False)
```

```python
import functools

import jax
import jax.numpy as jnp
from jax import lax
from jax.experimental import pallas as pl
from jax.experimental.pallas import tpu as pltpu
from jax.sharding import PartitionSpec as P


LEARN_RATE = 0.003
BETA_ONE = 0.9
BETA_TWO = 0.95
ADAM_EPS = 1e-8
WEIGHT_DECAY = 0.1
CLIP_NORM = 1.0
OPT_STEP = 10

ROW_STEP = 264
TOK_STEP = 512
ADAMW_DEPTH = 4
ADAMW_FLOPS = 2000
VMEM_LIMIT = 60 * 1024 * 1024


def dot_nt(a, b):
    return lax.dot_general(a, b, (((1,), (1,)), ((), ())), preferred_element_type=jnp.float32)


SPREAD_CHUNKS = 24
MESH = pl.DeviceIdType.MESH


def spread_kernel(act_ref, ids_ref, hid_ref, look_ref, all_ids_ref, buf, ids_buf, sx, sy, sz, sd, sl, si, load, recv, recv_core, recv_ids):
    z, y, p = lax.axis_index("tp"), lax.axis_index("dp"), lax.axis_index("pp")
    x, core, odd = p // 2, p % 2, z % 2
    x_dev = {"pp": (1 - x) * 2 + core}
    y_dev = {"dp": 1 - y}
    z_dev = {"tp": z + 1 - 2 * odd}
    core_dev = {"pp": x * 2 + 1 - core}
    plane = [{"dp": (y + dy) % 2, "pp": (p + dp) % 4} for dy in range(2) for dp in range(4) if dy + dp > 0]
    n = SPREAD_CHUNKS
    edge, main = n // 3, 2 * n // 3
    tok = act_ref.shape[0]
    size = tok // n

    barrier = pltpu.get_barrier_semaphore()
    for dev in plane + [z_dev]:
        pl.semaphore_signal(barrier, inc=1, device_id=dev, device_id_type=MESH)
    pl.semaphore_wait(barrier, len(plane) + 1)

    def chunk(i):
        if i < edge:
            return odd * main + i
        return i if i < main else (1 - odd) * main + (i - main)

    def span(replica, i):
        return pl.ds(pl.multiple_of(replica * tok + chunk(i) * size, size), size)

    def remote(src, dst, send_sem, recv_sem, dev):
        copy = pltpu.make_async_remote_copy(src_ref=src, dst_ref=dst, send_sem=send_sem, recv_sem=recv_sem, device_id=dev, device_id_type=MESH)
        copy.start()
        return copy

    def send_ids(kind):
        local = pltpu.make_async_copy(ids_ref, ids_buf.at[kind, y], recv_ids.at[kind, y])
        local.start()
        for i, dev in enumerate(plane):
            remote(ids_ref, ids_buf.at[kind, y], si.at[i], recv_ids.at[kind, y], dev)

    def drain_ids():
        for i in range(len(plane)):
            pltpu.make_async_copy(ids_ref, ids_ref, si.at[i]).wait()

    pl.when(p == 0)(lambda: send_ids(0))
    pl.when(p == 3)(lambda: send_ids(1))

    def run(out_ref, x_src):

        def send(replica, i, send_sem, recv_sem, dev):
            view = buf.at[span(replica, i)]
            return remote(view, view, send_sem, recv_sem, dev)

        def arrived(replica, i, slot):
            view = buf.at[span(replica, i)]
            pltpu.make_async_copy(view, view, recv.at[slot, i]).wait()

        def keep(copies, replica, i, slot):
            view, place = buf.at[span(replica, i)], out_ref.at[span(replica, i)]
            copies.append(remote(view, place, sd.at[slot, i], recv_core.at[slot, i], core_dev).wait_send)
            local = pltpu.make_async_copy(view, place, sl.at[slot, i])
            local.start()
            copies.append(local.wait)

        @pl.when(x == x_src)
        def _():
            copies, loads = [], []
            for i in range(n):
                rows = pl.ds(pl.multiple_of(chunk(i) * size, size), size)
                loads.append(pltpu.make_async_copy(act_ref.at[rows], buf.at[span(y, i)], load.at[i]))
                loads[-1].start()
            for i in range(n):
                loads[i].wait()
                if i < edge:
                    copies.append(send(y, i, sx.at[i], recv.at[0, i], x_dev).wait_send)
                if i < main:
                    copies.append(send(y, i, sy.at[i], recv.at[1, i], y_dev).wait_send)
            for i in range(n):
                keep(copies, y, i, 0)
            for i in range(main):
                arrived(1 - y, i, 1)
                if i + edge < main:
                    copies.append(send(y, i + edge, sx.at[i + edge], recv.at[0, i + edge], x_dev).wait_send)
                if i % 2 == 0:
                    copies.append(send(1 - y, i, sx.at[main + i // 2], recv.at[1, i], x_dev).wait_send)
                if i < edge:
                    copies.append(send(1 - y, i, sz.at[1, i], recv.at[1, main + i], z_dev).wait_send)
                keep(copies, 1 - y, i, 1)
            for i in range(main, n):
                arrived(1 - y, i, 1)
                keep(copies, 1 - y, i, 1)
            for wait in copies:
                wait()

        @pl.when(x != x_src)
        def _():
            copies = []
            for s in range(main + edge):
                if s < main:
                    arrived(y, s, 0)
                    if s % 2 == 1:
                        copies.append(send(y, s, sy.at[s], recv.at[1, s], y_dev).wait_send)
                    if s < edge:
                        copies.append(send(y, s, sz.at[0, s], recv.at[0, main + s], z_dev).wait_send)
                    keep(copies, y, s, 0)
                if s >= edge:
                    i = s - edge
                    arrived(1 - y, i, 1)
                    if i < edge:
                        copies.append(send(1 - y, i, sz.at[1, i], recv.at[1, main + i], z_dev).wait_send)
                    keep(copies, 1 - y, i, 1)
            for i in range(main, n):
                for slot, replica in ((0, y), (1, 1 - y)):
                    arrived(replica, i, slot)
                    keep(copies, replica, i, slot)
            for wait in copies:
                wait()

    def wait_core(out_ref):
        for slot, replica in ((0, y), (1, 1 - y)):
            for i in range(n):
                view = out_ref.at[span(replica, i)]
                pltpu.make_async_copy(view, view, recv_core.at[slot, i]).wait()

    @pl.when(core == 1)
    def _():
        run(hid_ref, 1)
        wait_core(look_ref)

    @pl.when(core == 0)
    def _():
        run(look_ref, 0)
        wait_core(hid_ref)

    for kind in range(2):
        for replica in range(2):
            pltpu.make_async_copy(ids_ref, ids_buf.at[kind, replica], recv_ids.at[kind, replica]).wait()
    pl.when(p == 0)(drain_ids)
    pl.when(p == 3)(drain_ids)
    all_ids_ref[...] = ids_buf[...]


def spread_call(acts, ids, n_repl):
    tok, dim = acts.shape
    n = SPREAD_CHUNKS
    shape = jax.ShapeDtypeStruct((n_repl * tok, dim), jnp.float32)
    ids_shape = (2, n_repl) + ids.shape
    dma = pltpu.SemaphoreType.DMA
    return pl.pallas_call(
        spread_kernel,
        in_specs=[pl.BlockSpec(memory_space=pl.ANY), pl.BlockSpec(memory_space=pltpu.VMEM)],
        out_specs=[pl.BlockSpec(memory_space=pl.ANY)] * 2 + [pl.BlockSpec(memory_space=pltpu.VMEM)],
        out_shape=[shape, shape, jax.ShapeDtypeStruct(ids_shape, jnp.int32)],
        scratch_shapes=[
            pltpu.VMEM((n_repl * tok, dim), jnp.float32), pltpu.VMEM(ids_shape, jnp.int32),
            dma((n + n // 2,)), dma((n,)), dma((2, n // 3)), dma((2, n)), dma((2, n)), dma((8,)),
            dma((n,)), dma((2, n)), dma((2, n)), dma((2, 2)),
        ],
        compiler_params=pltpu.CompilerParams(collective_id=0, has_side_effects=True, vmem_limit_bytes=VMEM_LIMIT),
        name="spread",
    )(acts, ids)


def slice_partners(z, y, p):
    return [
        {"pp": (p // 2) * 2 + 1 - p % 2}, {"pp": (1 - p // 2) * 2 + p % 2}, {"dp": 1 - y},
        {"tp": z + 1 - 2 * (z % 2)}, {"tp": (z + 2) % 4},
    ]


def meet(partners):
    barrier = pltpu.get_barrier_semaphore()
    for dev in partners:
        pl.semaphore_signal(barrier, inc=1, device_id=dev, device_id_type=MESH)
    pl.semaphore_wait(barrier, len(partners))


def combine_kernel(scale, in_ref, top_ref, inv_ref, mine, theirs, send_sem, recv_sem):
    z, y, p = lax.axis_index("tp"), lax.axis_index("dp"), lax.axis_index("pp")
    partners = slice_partners(z, y, p)
    meet(partners)
    half = in_ref.shape[0] // 2
    mine[0] = in_ref[...]
    for step, dev in enumerate(partners):
        copy = pltpu.make_async_remote_copy(src_ref=mine.at[step], dst_ref=theirs.at[step], send_sem=send_sem.at[step], recv_sem=recv_sem.at[step], device_id=dev, device_id_type=MESH)
        copy.start()
        copy.wait()
        top_a, sum_a = mine[step, :half], mine[step, half:]
        top_b, sum_b = theirs[step, :half], theirs[step, half:]
        top = jnp.maximum(top_a, top_b)
        total = sum_a * jnp.exp(top_a - top) + sum_b * jnp.exp(top_b - top)
        if step + 1 < len(partners):
            mine[step + 1, :half] = top
            mine[step + 1, half:] = total
        else:
            top_ref[...] = top
            inv_ref[...] = 1.0 / (total * scale)


def combine_call(local, scale):
    rows, lanes = local.shape
    shape = jax.ShapeDtypeStruct((rows // 2, lanes), jnp.float32)
    return pl.pallas_call(
        functools.partial(combine_kernel, scale),
        in_specs=[pl.BlockSpec(memory_space=pltpu.VMEM)],
        out_specs=[pl.BlockSpec(memory_space=pltpu.VMEM)] * 2,
        out_shape=[shape, shape],
        scratch_shapes=[pltpu.VMEM((5, rows, lanes), jnp.float32), pltpu.VMEM((5, rows, lanes), jnp.float32), pltpu.SemaphoreType.DMA((5,)), pltpu.SemaphoreType.DMA((5,))],
        compiler_params=pltpu.CompilerParams(collective_id=1, has_side_effects=True),
        name="combine",
    )(local)


def stats_kernel(scal_ref, master_ref, act_ref, max_ref, sum_ref, cast_ref, *table_refs):
    @pl.when(pl.program_id(0) == 0)
    def _():
        start = 0
        for ref in table_refs:
            ref[...] = master_ref[start:start + ref.shape[0], :].astype(jnp.bfloat16)
            start += ref.shape[0]

    act = act_ref[...].astype(jnp.bfloat16)
    cast_ref[...] = act
    rows = master_ref.shape[0]
    tiles = [ref[i:i + ROW_STEP, :] for ref in table_refs for i in range(0, ref.shape[0], ROW_STEP)]
    parts = []
    for start, tile in zip(range(0, rows, ROW_STEP), tiles):
        logits = dot_nt(tile, act)
        if start + ROW_STEP == rows:
            row = start + lax.broadcasted_iota(jnp.int32, logits.shape, 0)
            logits = jnp.where(row < scal_ref[1], logits, -jnp.inf)
        top = jnp.max(logits, axis=0, keepdims=True)
        parts.append((top, jnp.sum(jnp.exp(logits - top), axis=0, keepdims=True)))
    top_all = functools.reduce(jnp.maximum, [p[0] for p in parts])
    max_ref[...] = top_all
    sum_ref[...] = functools.reduce(jnp.add, [p[1] * jnp.exp(p[0] - top_all) for p in parts])


def stats_call(scal, master, splits, acts):
    tokens, dim = acts.shape
    rows = sum(splits)
    return pl.pallas_call(
        stats_kernel,
        grid_spec=pltpu.PrefetchScalarGridSpec(
            num_scalar_prefetch=1,
            grid=(tokens // TOK_STEP,),
            in_specs=[
                pl.BlockSpec((rows, dim), lambda t, scal: (scal[2], 0), pipeline_mode=pl.Buffered(1)),
                pl.BlockSpec((TOK_STEP, dim), lambda t, scal: (t, 0)),
            ],
            out_specs=[
                pl.BlockSpec((1, TOK_STEP), lambda t, scal: (0, t)),
                pl.BlockSpec((1, TOK_STEP), lambda t, scal: (0, t)),
                pl.BlockSpec((TOK_STEP, dim), lambda t, scal: (t, 0)),
            ] + [pl.BlockSpec((part, dim), lambda t, scal: (0, 0)) for part in splits],
        ),
        out_shape=[
            jax.ShapeDtypeStruct((1, tokens), jnp.float32),
            jax.ShapeDtypeStruct((1, tokens), jnp.float32),
            jax.ShapeDtypeStruct((tokens, dim), jnp.bfloat16),
        ] + [jax.ShapeDtypeStruct((part, dim), jnp.bfloat16) for part in splits],
        compiler_params=pltpu.CompilerParams(vmem_limit_bytes=VMEM_LIMIT),
        cost_estimate=pl.CostEstimate(flops=2 * tokens * rows * dim, bytes_accessed=6 * tokens * dim, transcendentals=tokens * rows),
        name="stats",
    )(scal, master, acts)


def norm_kernel(n_dev, *refs):
    *in_refs, out_ref, mine, theirs, send_sem, recv_sem = refs
    z, y, p = lax.axis_index("tp"), lax.axis_index("dp"), lax.axis_index("pp")
    n_tp, n_repl, n_stage = n_dev
    steps = [(a, b, c) for a in range(n_tp) for b in range(n_repl) for c in range(n_stage)][1:]
    devices = [{"tp": (z + a) % n_tp, "dp": (y + b) % n_repl, "pp": (p + c) % n_stage} for a, b, c in steps]
    meet(devices)
    mine[...] = jnp.full(mine.shape, jnp.sum(sum(ref[...] for ref in in_refs)))
    me = (z * n_repl + y) * n_stage + p
    copies = []
    for i, dev in enumerate(devices):
        copy = pltpu.make_async_remote_copy(src_ref=mine, dst_ref=theirs.at[me], send_sem=send_sem.at[i], recv_sem=recv_sem.at[me], device_id=dev, device_id_type=MESH)
        copy.start()
        copies.append(copy)
    own = pltpu.make_async_copy(mine, theirs.at[me], recv_sem.at[me])
    own.start()
    for i in range(len(steps) + 1):
        pltpu.make_async_copy(mine, theirs.at[i], recv_sem.at[i]).wait()
    for copy in copies:
        copy.wait_send()
    total = jnp.sum(theirs[...], axis=0)
    out_ref[...] = CLIP_NORM / jnp.maximum(jnp.sqrt(total), CLIP_NORM)


def norm_call(squares, n_dev):
    n_all = n_dev[0] * n_dev[1] * n_dev[2]
    vmem = pl.BlockSpec(memory_space=pltpu.VMEM)
    return pl.pallas_call(
        functools.partial(norm_kernel, n_dev),
        in_specs=[vmem] * len(squares),
        out_specs=vmem,
        out_shape=jax.ShapeDtypeStruct((8, 128), jnp.float32),
        scratch_shapes=[pltpu.VMEM((8, 128), jnp.float32), pltpu.VMEM((n_all, 8, 128), jnp.float32), pltpu.SemaphoreType.DMA((n_all,)), pltpu.SemaphoreType.DMA((n_all,))],
        compiler_params=pltpu.CompilerParams(collective_id=2, has_side_effects=True),
        name="norm",
    )(*squares)


def grad_kernel(offset, tok_count, scal_ref, table_ref, hid_ref, dx_ref, max_ref, inv_ref, lab_ref, ids_ref, *out_refs):
    *grad_refs, sq_ref = out_refs
    step = pl.program_id(0)
    rows = grad_refs[0].shape[0]

    @pl.when(step == 0)
    def _():
        for grad_ref in grad_refs:
            grad_ref[...] = jnp.zeros_like(grad_ref)

    hid = hid_ref[...]
    look = dx_ref[...].astype(jnp.bfloat16)
    for start in range(0, rows * len(grad_refs), ROW_STEP):
        logits = dot_nt(table_ref[start:start + ROW_STEP, :], hid)
        local = offset + start + lax.broadcasted_iota(jnp.int32, logits.shape, 0)
        row = jnp.where(local < scal_ref[1], local + scal_ref[0], -1)
        prob = jnp.where(local < scal_ref[1], jnp.exp(logits - max_ref[...]) * inv_ref[...], 0.0)
        dlog = (prob - jnp.where(row == lab_ref[...], 1.0 / tok_count, 0.0)).astype(jnp.bfloat16)
        hot = jnp.where(row == ids_ref[...], 1.0, 0.0).astype(jnp.bfloat16)
        part = jnp.dot(dlog, hid, preferred_element_type=jnp.float32)
        part += jnp.dot(hot, look, preferred_element_type=jnp.float32)
        grad_refs[start // rows][start % rows:start % rows + ROW_STEP, :] += part

    @pl.when(step == pl.num_programs(0) - 1)
    def _():
        square = jnp.zeros_like(sq_ref)
        for grad_ref in grad_refs:
            grad = grad_ref[...] * 0.5
            grad_ref[...] = grad
            square += jnp.sum(grad * grad, axis=0, keepdims=True)
        sq_ref[...] = square


def grad_call(scal, table_bf, hid, dx, top, inv, labels, ids, offset, tok_count):
    tokens, dim = hid.shape
    rows, n_out = table_bf.shape[0], 1
    tok_spec = pl.BlockSpec((1, TOK_STEP), lambda t: (0, t))
    act_spec = pl.BlockSpec((TOK_STEP, dim), lambda t: (t, 0))
    return pl.pallas_call(
        functools.partial(grad_kernel, offset, tok_count),
        grid=(tokens // TOK_STEP,),
        in_specs=[
            pl.BlockSpec(memory_space=pltpu.SMEM),
            pl.BlockSpec((rows * n_out, dim), lambda t: (0, 0)),
            act_spec, act_spec, tok_spec, tok_spec, tok_spec, tok_spec,
        ],
        out_specs=[pl.BlockSpec((rows, dim), lambda t: (0, 0))] * n_out + [pl.BlockSpec((1, dim), lambda t: (0, 0))],
        out_shape=[jax.ShapeDtypeStruct((rows, dim), jnp.float32)] * n_out + [jax.ShapeDtypeStruct((1, dim), jnp.float32)],
        compiler_params=pltpu.CompilerParams(vmem_limit_bytes=VMEM_LIMIT),
        cost_estimate=pl.CostEstimate(flops=6 * tokens * rows * n_out * dim, bytes_accessed=6 * tokens * dim, transcendentals=tokens * rows * n_out),
    )(scal, table_bf, hid, dx, top, inv, labels, ids)


def adamw_kernel(counts, spots, n_alias, *refs):
    n_piece = len(counts)
    scale_ref = refs[0]
    state_refs = refs[1:4]
    piece_refs = refs[4:4 + n_piece]
    *out_refs, out_scale, in_buf, out_buf, bf_buf, in_sem, out_sem = refs[4 + n_piece + n_alias:]
    y, p = lax.axis_index("dp"), lax.axis_index("pp")
    x, core = p // 2, p % 2
    out_scale[...] = scale_ref[...]
    scale = scale_ref[0:1, 0:1]
    vocab = state_refs[0].shape[0]
    depth, short, sub_rows = in_buf.shape[0], vocab % ROW_STEP, 24
    blocks = [(j, i) for j, count in enumerate(counts) for i in range(count)]

    def by_length(row, action):
        if short == 0:
            action(ROW_STEP)
        else:
            pl.when(row + ROW_STEP <= vocab)(lambda: action(ROW_STEP))
            pl.when(row + ROW_STEP > vocab)(lambda: action(short))

    def first_row(b):
        j, i = blocks[b]
        flip_y, flip_x, flip_core, block = spots[j]
        yy, xx, cc = (1 - v if flip else v for v, flip in ((y, flip_y), (x, flip_x), (core, flip_core)))
        own_blocks = -(-vocab // (8 * ROW_STEP))
        return pl.multiple_of(((yy * 4 + xx * 2 + cc) * own_blocks + block + i) * ROW_STEP, 8)

    def grad_copy(b):
        j, i = blocks[b]
        return pltpu.make_async_copy(piece_refs[j].at[pl.ds(i * ROW_STEP, ROW_STEP)], in_buf.at[b % depth, 3], in_sem.at[b % depth, 3])

    def in_copies(b, row, size):
        slot = b % depth
        return [pltpu.make_async_copy(ref.at[pl.ds(row, size)], in_buf.at[slot, k, pl.ds(0, size)], in_sem.at[slot, k]) for k, ref in enumerate(state_refs)]

    def out_copies(b, row, size):
        slot = b % depth
        sources = [out_buf.at[slot, k] for k in range(3)] + [bf_buf.at[slot]]
        return [pltpu.make_async_copy(src.at[pl.ds(0, size)], ref.at[pl.ds(row, size)], out_sem.at[slot, k]) for k, (src, ref) in enumerate(zip(sources, out_refs))]

    def each(make, b, method):
        row = first_row(b)

        def act(size):
            for copy in make(b, row, size):
                getattr(copy, method)()

        by_length(row, act)

    def start_in(b):
        each(in_copies, b, "start")
        grad_copy(b).start()

    for b in range(min(depth - 1, len(blocks))):
        start_in(b)
    for b in range(len(blocks)):
        if b + depth - 1 < len(blocks):
            start_in(b + depth - 1)
        each(in_copies, b, "wait")
        grad_copy(b).wait()
        if b >= depth:
            each(out_copies, b - depth, "wait")
        slot = b % depth

        def body(i, carry):
            rows = pl.ds(pl.multiple_of(i * sub_rows, 8), sub_rows)
            grad = in_buf[slot, 3, rows, :] * scale
            avg = BETA_ONE * in_buf[slot, 1, rows, :] + (1.0 - BETA_ONE) * grad
            sq = BETA_TWO * in_buf[slot, 2, rows, :] + (1.0 - BETA_TWO) * grad * grad
            step_dir = (avg / (1.0 - BETA_ONE ** OPT_STEP)) / (jnp.sqrt(sq / (1.0 - BETA_TWO ** OPT_STEP)) + ADAM_EPS)
            old = in_buf[slot, 0, rows, :]
            new = old - LEARN_RATE * (step_dir + WEIGHT_DECAY * old)
            out_buf[slot, 0, rows, :] = new
            out_buf[slot, 1, rows, :] = avg
            out_buf[slot, 2, rows, :] = sq
            bf_buf[slot, rows, :] = new.astype(jnp.bfloat16)
            return carry

        lax.fori_loop(0, ROW_STEP // sub_rows, body, 0)
        each(out_copies, b, "start")
    for b in range(max(0, len(blocks) - depth), len(blocks)):
        each(out_copies, b, "wait")


def adamw_call(scale, state, pieces, spots, outs):
    vocab, dim = state[0].shape
    counts = tuple(p.shape[0] // ROW_STEP for p in pieces)
    extra = list(outs) if outs is not None else []
    n_in = 1 + 3 + len(pieces)
    shapes = [jax.ShapeDtypeStruct((vocab, dim), jnp.float32)] * 3 + [jax.ShapeDtypeStruct((vocab, dim), jnp.bfloat16)]
    n_el = sum(counts) * ROW_STEP * dim
    hbm, vmem = pl.BlockSpec(memory_space=pl.ANY), pl.BlockSpec(memory_space=pltpu.VMEM)
    return pl.pallas_call(
        functools.partial(adamw_kernel, counts, spots, len(extra)),
        in_specs=[vmem] + [hbm] * (3 + len(pieces) + len(extra)),
        out_specs=[hbm] * 4 + [vmem],
        out_shape=shapes + [jax.ShapeDtypeStruct((8, 128), jnp.float32)],
        scratch_shapes=[
            pltpu.VMEM((ADAMW_DEPTH, 4, ROW_STEP, dim), jnp.float32), pltpu.VMEM((ADAMW_DEPTH, 3, ROW_STEP, dim), jnp.float32),
            pltpu.VMEM((ADAMW_DEPTH, ROW_STEP, dim), jnp.bfloat16), pltpu.SemaphoreType.DMA((ADAMW_DEPTH, 4)), pltpu.SemaphoreType.DMA((ADAMW_DEPTH, 4)),
        ],
        input_output_aliases={n_in + i: i for i in range(len(extra))},
        compiler_params=pltpu.CompilerParams(vmem_limit_bytes=VMEM_LIMIT),
        cost_estimate=pl.CostEstimate(flops=ADAMW_FLOPS * n_el, bytes_accessed=30 * n_el, transcendentals=n_el),
    )(scale, *state, *pieces, *extra)


def solution(mesh):
    n_stage, n_repl, n_tp = mesh.shape["pp"], mesh.shape["dp"], mesh.shape["tp"]
    n_plane = n_stage * n_repl
    table_spec = P("tp", None)
    axes = ("tp", "dp", "pp")
    x_swap = [(i, i ^ 2) for i in range(n_stage)]
    core_swap = [(i, i ^ 1) for i in range(n_stage)]
    y_swap = [(0, 1), (1, 0)]
    corner_pairs = [(yy * n_stage + q, (1 - yy) * n_stage + q if q % 2 == 0 else yy * n_stage + (q ^ 2)) for yy in range(n_repl) for q in range(n_stage)]

    def device_step(master, exp_avg, exp_avg_sq, stage_ids, stage_acts):
        z, y, p = (lax.axis_index(a) for a in axes)
        vocab, dim = master.shape
        tok = stage_ids.shape[1] * stage_ids.shape[2]
        own_rows = -(-vocab // (n_plane * 6 * ROW_STEP)) * 6 * ROW_STEP
        plane = y * n_stage + p

        first_row = plane * own_rows
        valid = jnp.minimum(own_rows, vocab - first_row)
        scal = jnp.stack([z * vocab + first_row, valid, plane]).astype(jnp.int32)

        acts = stage_acts.reshape(tok, dim).astype(jnp.float32)
        hid, dx, all_ids = spread_call(acts, stage_ids.reshape(tok // 128, 128), n_repl)
        ids, labels = all_ids[0].reshape(1, -1), all_ids[1].reshape(1, -1)
        rows_a = own_rows // (2 * ROW_STEP) * ROW_STEP
        top_own, sum_own, hid_bf, table_a, table_b = stats_call(scal, master, (rows_a, own_rows - rows_a), hid)
        local = jnp.concatenate([top_own.reshape(-1, 128), sum_own.reshape(-1, 128)], axis=0)
        top, inv = (a.reshape(1, -1) for a in combine_call(local, float(tok)))

        n_block = own_rows // ROW_STEP
        start_b = rows_a // ROW_STEP
        part_a, sq_a = grad_call(scal, table_a, hid_bf, dx, top, inv, labels, ids, 0, tok)
        part_b, sq_b = grad_call(scal, table_b, hid_bf, dx, top, inv, labels, ids, rows_a, tok)
        scale = norm_call([sq_a, sq_b], (n_tp, n_repl, n_stage))
        part_b, scale = lax.optimization_barrier((part_b, scale))

        def across(a):
            return lax.ppermute(a, "pp", core_swap)

        def direct(a):
            from_x = lax.ppermute(a, "pp", x_swap)
            return from_x, lax.ppermute(a, "dp", y_swap)

        def corner(from_x, from_y):
            payload = jnp.where(p % 2 == 0, from_x, from_y)
            return lax.ppermute(payload, ("dp", "pp"), corner_pairs)

        def call(pieces, outs, scale):
            *outs, scale = adamw_call(scale, (master, exp_avg, exp_avg_sq), [a for a, _ in pieces], tuple(spot for _, spot in pieces), outs)
            return outs, scale

        def direct_pieces(arrays, c):
            spots = ((False, True), (True, False))
            return [(a, (*spot, False, c)) for a, spot in zip(arrays, spots)] + [(across(a), (*spot, True, c)) for a, spot in zip(arrays, spots)]

        def corner_pieces(array, c):
            return [(array, (True, True, False, c)), (across(array), (True, True, True, c))]

        def own(other_core, c):
            return (False, False, other_core, c)

        sent_a, sent_b = direct(part_a), direct(part_b)
        cross_a, cross_b = across(part_a), across(part_b)
        direct_a = direct_pieces(sent_a, 0)
        far_a = corner(*sent_a)
        outs, scale = call([(part_a, own(False, 0)), (part_b, own(False, start_b)), (cross_a, own(True, 0))], None, scale)
        outs, scale = call(direct_a + [(cross_b, own(True, start_b))], outs, scale)
        far_a, scale = lax.optimization_barrier((far_a, scale))
        outs, scale = call(corner_pieces(far_a, 0), outs, scale)
        sent_b, scale = lax.optimization_barrier((sent_b, scale))
        cut = (n_block - start_b + 1) // 2 * ROW_STEP
        far_b = [corner(*(a[:cut] for a in sent_b)), corner(*(a[cut:] for a in sent_b))]
        outs, scale = call(direct_pieces(sent_b, start_b), outs, scale)
        for i, c in enumerate((start_b, start_b + cut // ROW_STEP)):
            far, scale = lax.optimization_barrier((far_b[i], scale))
            outs, scale = call(corner_pieces(far, c), outs, scale)
        return tuple(outs)

    return jax.shard_map(device_step, mesh=mesh, in_specs=(table_spec, table_spec, table_spec, P("pp", "dp", None), P("pp", "dp", None, None)), out_specs=(table_spec, table_spec, table_spec, table_spec), check_vma=False)
```

```python
import functools

import jax
import jax.numpy as jnp
from jax import lax
from jax.experimental import pallas as pl
from jax.experimental.pallas import tpu as pltpu
from jax.sharding import PartitionSpec as P


LEARN_RATE = 0.003
BETA_ONE = 0.9
BETA_TWO = 0.95
ADAM_EPS = 1e-8
WEIGHT_DECAY = 0.1
CLIP_NORM = 1.0
OPT_STEP = 10

ROW_STEP = 264
TOK_STEP = 512
ADAMW_DEPTH = 4
ADAMW_FLOPS = 2000
VMEM_LIMIT = 60 * 1024 * 1024


def dot_nt(a, b):
    return lax.dot_general(a, b, (((1,), (1,)), ((), ())), preferred_element_type=jnp.float32)


SPREAD_CHUNKS = 24
MESH = pl.DeviceIdType.MESH


def spread_kernel(rows_valid, act_ref, ids_ref, master_ref, hid_ref, look_ref, all_ids_ref, table_ref, top_ref, sum_ref,
                  buf, hid_buf, master_buf, ids_buf, sx, sy, sz, sd, sl, so, si, load, sm, recv, recv_core, recv_ids):
    z, y, p = lax.axis_index("tp"), lax.axis_index("dp"), lax.axis_index("pp")
    x, core, odd = p // 2, p % 2, z % 2
    is_src = x == core
    x_dev = {"pp": (1 - x) * 2 + core}
    y_dev = {"dp": 1 - y}
    z_dev = {"tp": z + 1 - 2 * odd}
    core_dev = {"pp": x * 2 + 1 - core}
    plane = [{"dp": (y + dy) % 2, "pp": (p + dp) % 4} for dy in range(2) for dp in range(4) if dy + dp > 0]
    n = SPREAD_CHUNKS
    edge, main, lag, unit = n // 3, 2 * n // 3, 3, 4
    tok = act_ref.shape[0]
    size = tok // n
    rows = table_ref.shape[0]
    device = y * 4 + p
    last = len(plane)
    meet(plane + [z_dev])

    def chunk(i):
        if i < edge:
            return odd * main + i
        return i if i < main else (1 - odd) * main + (i - main)

    def span(slot, i, count=1):
        replica = y if slot == 0 else 1 - y
        return pl.ds(pl.multiple_of(replica * tok + chunk(i) * size, size), size * count)

    def remote(src, dst, send_sem, recv_sem, dev):
        pltpu.make_async_remote_copy(src_ref=src, dst_ref=dst, send_sem=send_sem, recv_sem=recv_sem, device_id=dev, device_id_type=MESH).start()

    def send(slot, i, send_sem, recv_sem, dev):
        view = buf.at[core, span(slot, i)]
        remote(view, view, send_sem, recv_sem, dev)

    def drain(sem):
        view = buf.at[0, pl.ds(0, size)]
        pltpu.make_async_copy(view, view, sem).wait()

    def arrived(slot, i):
        drain(recv.at[slot, i])

    def keep(slot, i):
        send(slot, i, sd.at[slot, i], recv_core.at[slot, i], core_dev)

    def send_ids(kind):
        pltpu.make_async_copy(ids_ref, ids_buf.at[kind, y], recv_ids.at[kind, y]).start()
        for i, dev in enumerate(plane):
            remote(ids_ref, ids_buf.at[kind, y], si.at[i], recv_ids.at[kind, y], dev)

    pl.when(p == 0)(lambda: send_ids(0))
    pl.when(p == 3)(lambda: send_ids(1))

    def master_copy(count):
        return pltpu.make_async_copy(master_ref.at[pl.ds(pl.multiple_of(device * rows, 8), count)], master_buf.at[pl.ds(0, count)], sm.at[0])

    pl.when(device < last)(lambda: master_copy(rows).start())

    @pl.when(device == last)
    def _():
        master_copy(rows_valid).start()
        if rows_valid < rows:
            master_buf[rows_valid:, :] = jnp.zeros((rows - rows_valid, master_buf.shape[1]), jnp.float32)

    @pl.when(is_src)
    def _():
        def load_copy(i):
            place = pl.ds(pl.multiple_of(chunk(i) * size, size), size)
            return pltpu.make_async_copy(act_ref.at[place], buf.at[core, span(0, i)], load.at[i])

        for i in range(n):
            load_copy(i).start()
        for i in range(n):
            load_copy(i).wait()
            if i < edge:
                send(0, i, sx.at[i], recv.at[0, i], x_dev)
            if i < main:
                send(0, i, sy.at[i], recv.at[1, i], y_dev)
        for i in range(n):
            keep(0, i)

    pl.when(device < last)(lambda: master_copy(rows).wait())
    pl.when(device == last)(lambda: master_copy(rows_valid).wait())
    table_ref[...] = master_buf[...].astype(jnp.bfloat16)
    valid = jnp.where(device == last, rows_valid, rows)

    def statistics(slot, i):
        place = span(slot, i, unit)
        act = buf[1, place, :].astype(jnp.bfloat16)
        hid_buf[place, :] = act
        pltpu.make_async_copy(hid_buf.at[place], hid_ref.at[place], so.at[slot, i // unit]).start()

        def tile(r, carry):
            top, total = carry
            start = pl.multiple_of(r * ROW_STEP, 8)
            logits = dot_nt(table_ref[pl.ds(start, ROW_STEP), :], act)
            row = start + lax.broadcasted_iota(jnp.int32, logits.shape, 0)
            logits = jnp.where(row < valid, logits, -jnp.inf)
            new_top = jnp.maximum(top, jnp.max(logits, axis=0, keepdims=True))
            return new_top, total * jnp.exp(top - new_top) + jnp.sum(jnp.exp(logits - new_top), axis=0, keepdims=True)

        empty = jnp.full((1, size * unit), -jnp.inf, jnp.float32)
        top, total = lax.fori_loop(0, rows // ROW_STEP, tile, (empty, jnp.zeros_like(empty)))
        where = pl.ds((y if slot == 0 else 1 - y) * (n // unit) + chunk(i) // unit, 1)
        top_ref[where, :] = top
        sum_ref[where, :] = total

    def ready(slot, i):
        drain(recv_core.at[slot, i])
        place = span(slot, i)
        pltpu.make_async_copy(buf.at[0, place], look_ref.at[place], sl.at[slot, i]).start()
        if i % unit == unit - 1:
            statistics(slot, i - unit + 1)

    def source_step(s):
        arrived(1, s)
        if s + edge < main:
            send(0, s + edge, sx.at[s + edge], recv.at[0, s + edge], x_dev)
        if s % 2 == 0:
            send(1, s, sx.at[main + s // 2], recv.at[1, s], x_dev)
        if s < edge:
            send(1, s, sz.at[1, s], recv.at[1, main + s], z_dev)
        keep(1, s)

    def other_step(s):
        if s < main:
            arrived(0, s)
            if s % 2 == 1:
                send(0, s, sy.at[s], recv.at[1, s], y_dev)
            if s < edge:
                send(0, s, sz.at[0, s], recv.at[0, main + s], z_dev)
            keep(0, s)
        i = s - edge
        if i >= 0:
            arrived(1, i)
            if i < edge:
                send(1, i, sz.at[1, i], recv.at[1, main + i], z_dev)
            keep(1, i)

    def take_far(slot, i):
        arrived(slot, i)
        keep(slot, i)

    done = set()

    def ready_once(slot, i):
        if 0 <= i and (slot, i) not in done:
            done.add((slot, i))
            ready(slot, i)

    for s in range(main + edge):
        far = main + (s - 4) // 2 if s >= 4 and s % 2 == 0 and (s - 4) // 2 < edge else None

        @pl.when(is_src)
        def _():
            if s < main:
                source_step(s)
            if far is not None:
                take_far(1, far)

        @pl.when(jnp.logical_not(is_src))
        def _():
            other_step(s)
            if far is not None:
                take_far(0, far)

        if s - lag < main:
            ready_once(0, s - lag)
        if s - edge - lag < main:
            ready_once(1, s - edge - lag)
        j = s - 4 - lag
        if j >= 0 and j % 2 == 0 and j // 2 < edge:
            ready_once(0, main + j // 2)

    @pl.when(jnp.logical_not(is_src))
    def _():
        for i in range(main, n):
            take_far(1, i)

    for slot in range(2):
        for i in range(n):
            ready_once(slot, i)

    for i in range(main):
        if i % 2 == 1:
            drain(sy.at[i])
    for i in range(edge):
        drain(sz.at[1, i])
    for slot in range(2):
        for i in range(n):
            drain(sd.at[slot, i])
            drain(sl.at[slot, i])
        for i in range(n // unit):
            view = hid_buf.at[pl.ds(0, size * unit)]
            pltpu.make_async_copy(view, view, so.at[slot, i]).wait()

    @pl.when(is_src)
    def _():
        for i in range(main + main // 2):
            drain(sx.at[i])
        for i in range(0, main, 2):
            drain(sy.at[i])

    @pl.when(jnp.logical_not(is_src))
    def _():
        for i in range(edge):
            drain(sz.at[0, i])

    for kind in range(2):
        for replica in range(2):
            pltpu.make_async_copy(ids_ref, ids_buf.at[kind, replica], recv_ids.at[kind, replica]).wait()

    @pl.when(jnp.logical_or(p == 0, p == 3))
    def _():
        for i in range(len(plane)):
            pltpu.make_async_copy(ids_ref, ids_ref, si.at[i]).wait()

    all_ids_ref[...] = ids_buf[...]


def spread_call(acts, ids, master, rows, n_repl):
    tok, dim = acts.shape
    n, unit = SPREAD_CHUNKS, 4
    ids_shape = (2, n_repl) + ids.shape
    dma = pltpu.SemaphoreType.DMA
    hbm, vmem = pl.BlockSpec(memory_space=pl.ANY), pl.BlockSpec(memory_space=pltpu.VMEM)
    stat = jax.ShapeDtypeStruct((n_repl * n // unit, tok // n * unit), jnp.float32)
    return pl.pallas_call(
        functools.partial(spread_kernel, master.shape[0] - 7 * rows),
        in_specs=[hbm, vmem, hbm],
        out_specs=[hbm, hbm, vmem, vmem, vmem, vmem],
        out_shape=[
            jax.ShapeDtypeStruct((n_repl * tok, dim), jnp.bfloat16), jax.ShapeDtypeStruct((n_repl * tok, dim), jnp.float32),
            jax.ShapeDtypeStruct(ids_shape, jnp.int32), jax.ShapeDtypeStruct((rows, dim), jnp.bfloat16), stat, stat,
        ],
        scratch_shapes=[
            pltpu.VMEM((2, n_repl * tok, dim), jnp.float32), pltpu.VMEM((n_repl * tok, dim), jnp.bfloat16), pltpu.VMEM((rows, dim), jnp.float32),
            pltpu.VMEM(ids_shape, jnp.int32),
            dma((n + n // 2,)), dma((n,)), dma((2, n // 3)), dma((2, n)), dma((2, n)), dma((2, n // unit)), dma((8,)),
            dma((n,)), dma((1,)), dma((2, n)), dma((2, n)), dma((2, 2)),
        ],
        compiler_params=pltpu.CompilerParams(collective_id=0, has_side_effects=True, vmem_limit_bytes=VMEM_LIMIT),
        name="spread",
    )(acts, ids, master)


def slice_partners(z, y, p):
    return [
        {"pp": (p // 2) * 2 + 1 - p % 2}, {"pp": (1 - p // 2) * 2 + p % 2}, {"dp": 1 - y},
        {"tp": z + 1 - 2 * (z % 2)}, {"tp": (z + 2) % 4},
    ]


def meet(partners):
    barrier = pltpu.get_barrier_semaphore()
    for dev in partners:
        pl.semaphore_signal(barrier, inc=1, device_id=dev, device_id_type=MESH)
    pl.semaphore_wait(barrier, len(partners))


def combine_kernel(scale, in_ref, top_ref, inv_ref, mine, theirs, send_sem, recv_sem):
    z, y, p = lax.axis_index("tp"), lax.axis_index("dp"), lax.axis_index("pp")
    partners = slice_partners(z, y, p)
    meet(partners)
    half = in_ref.shape[0] // 2
    mine[0] = in_ref[...]
    for step, dev in enumerate(partners):
        copy = pltpu.make_async_remote_copy(src_ref=mine.at[step], dst_ref=theirs.at[step], send_sem=send_sem.at[step], recv_sem=recv_sem.at[step], device_id=dev, device_id_type=MESH)
        copy.start()
        copy.wait()
        top_a, sum_a = mine[step, :half], mine[step, half:]
        top_b, sum_b = theirs[step, :half], theirs[step, half:]
        top = jnp.maximum(top_a, top_b)
        total = sum_a * jnp.exp(top_a - top) + sum_b * jnp.exp(top_b - top)
        if step + 1 < len(partners):
            mine[step + 1, :half] = top
            mine[step + 1, half:] = total
        else:
            top_ref[...] = top
            inv_ref[...] = 1.0 / (total * scale)


def combine_call(local, scale):
    rows, lanes = local.shape
    shape = jax.ShapeDtypeStruct((rows // 2, lanes), jnp.float32)
    return pl.pallas_call(
        functools.partial(combine_kernel, scale),
        in_specs=[pl.BlockSpec(memory_space=pltpu.VMEM)],
        out_specs=[pl.BlockSpec(memory_space=pltpu.VMEM)] * 2,
        out_shape=[shape, shape],
        scratch_shapes=[pltpu.VMEM((5, rows, lanes), jnp.float32), pltpu.VMEM((5, rows, lanes), jnp.float32), pltpu.SemaphoreType.DMA((5,)), pltpu.SemaphoreType.DMA((5,))],
        compiler_params=pltpu.CompilerParams(collective_id=1, has_side_effects=True),
        name="combine",
    )(local)


def norm_kernel(n_dev, *refs):
    *in_refs, out_ref, mine, theirs, send_sem, recv_sem = refs
    z, y, p = lax.axis_index("tp"), lax.axis_index("dp"), lax.axis_index("pp")
    n_tp, n_repl, n_stage = n_dev
    steps = [(a, b, c) for a in range(n_tp) for b in range(n_repl) for c in range(n_stage)][1:]
    devices = [{"tp": (z + a) % n_tp, "dp": (y + b) % n_repl, "pp": (p + c) % n_stage} for a, b, c in steps]
    meet(devices)
    mine[...] = jnp.full(mine.shape, jnp.sum(sum(ref[...] for ref in in_refs)))
    me = (z * n_repl + y) * n_stage + p
    copies = []
    for i, dev in enumerate(devices):
        copy = pltpu.make_async_remote_copy(src_ref=mine, dst_ref=theirs.at[me], send_sem=send_sem.at[i], recv_sem=recv_sem.at[me], device_id=dev, device_id_type=MESH)
        copy.start()
        copies.append(copy)
    own = pltpu.make_async_copy(mine, theirs.at[me], recv_sem.at[me])
    own.start()
    for i in range(len(steps) + 1):
        pltpu.make_async_copy(mine, theirs.at[i], recv_sem.at[i]).wait()
    for copy in copies:
        copy.wait_send()
    total = jnp.sum(theirs[...], axis=0)
    out_ref[...] = CLIP_NORM / jnp.maximum(jnp.sqrt(total), CLIP_NORM)


def norm_call(squares, n_dev):
    n_all = n_dev[0] * n_dev[1] * n_dev[2]
    vmem = pl.BlockSpec(memory_space=pltpu.VMEM)
    return pl.pallas_call(
        functools.partial(norm_kernel, n_dev),
        in_specs=[vmem] * len(squares),
        out_specs=vmem,
        out_shape=jax.ShapeDtypeStruct((8, 128), jnp.float32),
        scratch_shapes=[pltpu.VMEM((8, 128), jnp.float32), pltpu.VMEM((n_all, 8, 128), jnp.float32), pltpu.SemaphoreType.DMA((n_all,)), pltpu.SemaphoreType.DMA((n_all,))],
        compiler_params=pltpu.CompilerParams(collective_id=2, has_side_effects=True),
        name="norm",
    )(*squares)


def grad_kernel(offset, tok_count, scal_ref, table_ref, hid_ref, dx_ref, max_ref, inv_ref, lab_ref, ids_ref, *out_refs):
    *grad_refs, sq_ref = out_refs
    step = pl.program_id(0)
    rows = grad_refs[0].shape[0]

    @pl.when(step == 0)
    def _():
        for grad_ref in grad_refs:
            grad_ref[...] = jnp.zeros_like(grad_ref)

    hid = hid_ref[...]
    look = dx_ref[...].astype(jnp.bfloat16)
    for start in range(0, rows * len(grad_refs), ROW_STEP):
        logits = dot_nt(table_ref[start:start + ROW_STEP, :], hid)
        local = offset + start + lax.broadcasted_iota(jnp.int32, logits.shape, 0)
        row = jnp.where(local < scal_ref[1], local + scal_ref[0], -1)
        prob = jnp.where(local < scal_ref[1], jnp.exp(logits - max_ref[...]) * inv_ref[...], 0.0)
        dlog = (prob - jnp.where(row == lab_ref[...], 1.0 / tok_count, 0.0)).astype(jnp.bfloat16)
        hot = jnp.where(row == ids_ref[...], 1.0, 0.0).astype(jnp.bfloat16)
        part = jnp.dot(dlog, hid, preferred_element_type=jnp.float32)
        part += jnp.dot(hot, look, preferred_element_type=jnp.float32)
        grad_refs[start // rows][start % rows:start % rows + ROW_STEP, :] += part

    @pl.when(step == pl.num_programs(0) - 1)
    def _():
        square = jnp.zeros_like(sq_ref)
        for grad_ref in grad_refs:
            grad = grad_ref[...] * 0.5
            grad_ref[...] = grad
            square += jnp.sum(grad * grad, axis=0, keepdims=True)
        sq_ref[...] = square


def grad_call(scal, table_bf, hid, dx, top, inv, labels, ids, offset, tok_count):
    tokens, dim = hid.shape
    rows, n_out = table_bf.shape[0] // 2, 1
    half = offset // rows
    tok_spec = pl.BlockSpec((1, TOK_STEP), lambda t: (0, t))
    act_spec = pl.BlockSpec((TOK_STEP, dim), lambda t: (t, 0))
    return pl.pallas_call(
        functools.partial(grad_kernel, offset, tok_count),
        grid=(tokens // TOK_STEP,),
        in_specs=[
            pl.BlockSpec(memory_space=pltpu.SMEM),
            pl.BlockSpec((rows * n_out, dim), lambda t: (half, 0)),
            act_spec, act_spec, tok_spec, tok_spec, tok_spec, tok_spec,
        ],
        out_specs=[pl.BlockSpec((rows, dim), lambda t: (0, 0))] * n_out + [pl.BlockSpec((1, dim), lambda t: (0, 0))],
        out_shape=[jax.ShapeDtypeStruct((rows, dim), jnp.float32)] * n_out + [jax.ShapeDtypeStruct((1, dim), jnp.float32)],
        compiler_params=pltpu.CompilerParams(vmem_limit_bytes=VMEM_LIMIT),
        cost_estimate=pl.CostEstimate(flops=6 * tokens * rows * n_out * dim, bytes_accessed=6 * tokens * dim, transcendentals=tokens * rows * n_out),
    )(scal, table_bf, hid, dx, top, inv, labels, ids)


def adamw_kernel(counts, spots, n_alias, *refs):
    n_piece = len(counts)
    scale_ref = refs[0]
    state_refs = refs[1:4]
    piece_refs = refs[4:4 + n_piece]
    *out_refs, out_scale, in_buf, out_buf, bf_buf, in_sem, out_sem = refs[4 + n_piece + n_alias:]
    y, p = lax.axis_index("dp"), lax.axis_index("pp")
    x, core = p // 2, p % 2
    out_scale[...] = scale_ref[...]
    scale = scale_ref[0:1, 0:1]
    vocab = state_refs[0].shape[0]
    depth, short, sub_rows = in_buf.shape[0], vocab % ROW_STEP, 24
    blocks = [(j, i) for j, count in enumerate(counts) for i in range(count)]

    def by_length(row, action):
        if short == 0:
            action(ROW_STEP)
        else:
            pl.when(row + ROW_STEP <= vocab)(lambda: action(ROW_STEP))
            pl.when(row + ROW_STEP > vocab)(lambda: action(short))

    def first_row(b):
        j, i = blocks[b]
        flip_y, flip_x, flip_core, block = spots[j]
        yy, xx, cc = (1 - v if flip else v for v, flip in ((y, flip_y), (x, flip_x), (core, flip_core)))
        own_blocks = -(-vocab // (8 * ROW_STEP))
        return pl.multiple_of(((yy * 4 + xx * 2 + cc) * own_blocks + block + i) * ROW_STEP, 8)

    def grad_copy(b):
        j, i = blocks[b]
        return pltpu.make_async_copy(piece_refs[j].at[pl.ds(i * ROW_STEP, ROW_STEP)], in_buf.at[b % depth, 3], in_sem.at[b % depth, 3])

    def in_copies(b, row, size):
        slot = b % depth
        return [pltpu.make_async_copy(ref.at[pl.ds(row, size)], in_buf.at[slot, k, pl.ds(0, size)], in_sem.at[slot, k]) for k, ref in enumerate(state_refs)]

    def out_copies(b, row, size):
        slot = b % depth
        sources = [out_buf.at[slot, k] for k in range(3)] + [bf_buf.at[slot]]
        return [pltpu.make_async_copy(src.at[pl.ds(0, size)], ref.at[pl.ds(row, size)], out_sem.at[slot, k]) for k, (src, ref) in enumerate(zip(sources, out_refs))]

    def each(make, b, method):
        row = first_row(b)

        def act(size):
            for copy in make(b, row, size):
                getattr(copy, method)()

        by_length(row, act)

    def start_in(b):
        each(in_copies, b, "start")
        grad_copy(b).start()

    for b in range(min(depth - 1, len(blocks))):
        start_in(b)
    for b in range(len(blocks)):
        if b + depth - 1 < len(blocks):
            start_in(b + depth - 1)
        each(in_copies, b, "wait")
        grad_copy(b).wait()
        if b >= depth:
            each(out_copies, b - depth, "wait")
        slot = b % depth

        def body(i, carry):
            rows = pl.ds(pl.multiple_of(i * sub_rows, 8), sub_rows)
            grad = in_buf[slot, 3, rows, :] * scale
            avg = BETA_ONE * in_buf[slot, 1, rows, :] + (1.0 - BETA_ONE) * grad
            sq = BETA_TWO * in_buf[slot, 2, rows, :] + (1.0 - BETA_TWO) * grad * grad
            step_dir = (avg / (1.0 - BETA_ONE ** OPT_STEP)) / (jnp.sqrt(sq / (1.0 - BETA_TWO ** OPT_STEP)) + ADAM_EPS)
            old = in_buf[slot, 0, rows, :]
            new = old - LEARN_RATE * (step_dir + WEIGHT_DECAY * old)
            out_buf[slot, 0, rows, :] = new
            out_buf[slot, 1, rows, :] = avg
            out_buf[slot, 2, rows, :] = sq
            bf_buf[slot, rows, :] = new.astype(jnp.bfloat16)
            return carry

        lax.fori_loop(0, ROW_STEP // sub_rows, body, 0)
        each(out_copies, b, "start")
    for b in range(max(0, len(blocks) - depth), len(blocks)):
        each(out_copies, b, "wait")


def adamw_call(scale, state, pieces, spots, outs):
    vocab, dim = state[0].shape
    counts = tuple(p.shape[0] // ROW_STEP for p in pieces)
    extra = list(outs) if outs is not None else []
    n_in = 1 + 3 + len(pieces)
    shapes = [jax.ShapeDtypeStruct((vocab, dim), jnp.float32)] * 3 + [jax.ShapeDtypeStruct((vocab, dim), jnp.bfloat16)]
    n_el = sum(counts) * ROW_STEP * dim
    hbm, vmem = pl.BlockSpec(memory_space=pl.ANY), pl.BlockSpec(memory_space=pltpu.VMEM)
    return pl.pallas_call(
        functools.partial(adamw_kernel, counts, spots, len(extra)),
        in_specs=[vmem] + [hbm] * (3 + len(pieces) + len(extra)),
        out_specs=[hbm] * 4 + [vmem],
        out_shape=shapes + [jax.ShapeDtypeStruct((8, 128), jnp.float32)],
        scratch_shapes=[
            pltpu.VMEM((ADAMW_DEPTH, 4, ROW_STEP, dim), jnp.float32), pltpu.VMEM((ADAMW_DEPTH, 3, ROW_STEP, dim), jnp.float32),
            pltpu.VMEM((ADAMW_DEPTH, ROW_STEP, dim), jnp.bfloat16), pltpu.SemaphoreType.DMA((ADAMW_DEPTH, 4)), pltpu.SemaphoreType.DMA((ADAMW_DEPTH, 4)),
        ],
        input_output_aliases={n_in + i: i for i in range(len(extra))},
        compiler_params=pltpu.CompilerParams(vmem_limit_bytes=VMEM_LIMIT),
        cost_estimate=pl.CostEstimate(flops=ADAMW_FLOPS * n_el, bytes_accessed=30 * n_el, transcendentals=n_el),
    )(scale, *state, *pieces, *extra)


def solution(mesh):
    n_stage, n_repl, n_tp = mesh.shape["pp"], mesh.shape["dp"], mesh.shape["tp"]
    n_plane = n_stage * n_repl
    table_spec = P("tp", None)
    axes = ("tp", "dp", "pp")
    x_swap = [(i, i ^ 2) for i in range(n_stage)]
    core_swap = [(i, i ^ 1) for i in range(n_stage)]
    y_swap = [(0, 1), (1, 0)]
    corner_pairs = [(yy * n_stage + q, (1 - yy) * n_stage + q if q % 2 == 0 else yy * n_stage + (q ^ 2)) for yy in range(n_repl) for q in range(n_stage)]

    def device_step(master, exp_avg, exp_avg_sq, stage_ids, stage_acts):
        z, y, p = (lax.axis_index(a) for a in axes)
        vocab, dim = master.shape
        tok = stage_ids.shape[1] * stage_ids.shape[2]
        own_rows = -(-vocab // (n_plane * 6 * ROW_STEP)) * 6 * ROW_STEP
        plane = y * n_stage + p

        first_row = plane * own_rows
        valid = jnp.minimum(own_rows, vocab - first_row)
        scal = jnp.stack([z * vocab + first_row, valid]).astype(jnp.int32)

        acts = stage_acts.reshape(tok, dim).astype(jnp.float32)
        hid_bf, dx, all_ids, table_bf, top_own, sum_own = spread_call(acts, stage_ids.reshape(tok // 128, 128), master, own_rows, n_repl)
        ids, labels = all_ids[0].reshape(1, -1), all_ids[1].reshape(1, -1)
        rows_a = own_rows // (2 * ROW_STEP) * ROW_STEP
        local = jnp.concatenate([top_own.reshape(-1, 128), sum_own.reshape(-1, 128)], axis=0)
        top, inv = (a.reshape(1, -1) for a in combine_call(local, float(tok)))

        n_block = own_rows // ROW_STEP
        start_b = rows_a // ROW_STEP
        part_a, sq_a = grad_call(scal, table_bf, hid_bf, dx, top, inv, labels, ids, 0, tok)
        part_b, sq_b = grad_call(scal, table_bf, hid_bf, dx, top, inv, labels, ids, rows_a, tok)
        scale = norm_call([sq_a, sq_b], (n_tp, n_repl, n_stage))
        part_b, scale = lax.optimization_barrier((part_b, scale))

        def across(a):
            return lax.ppermute(a, "pp", core_swap)

        def direct(a):
            from_x = lax.ppermute(a, "pp", x_swap)
            return from_x, lax.ppermute(a, "dp", y_swap)

        def corner(from_x, from_y):
            payload = jnp.where(p % 2 == 0, from_x, from_y)
            return lax.ppermute(payload, ("dp", "pp"), corner_pairs)

        def call(pieces, outs, scale):
            *outs, scale = adamw_call(scale, (master, exp_avg, exp_avg_sq), [a for a, _ in pieces], tuple(spot for _, spot in pieces), outs)
            return outs, scale

        def direct_pieces(arrays, c):
            spots = ((False, True), (True, False))
            return [(a, (*spot, False, c)) for a, spot in zip(arrays, spots)] + [(across(a), (*spot, True, c)) for a, spot in zip(arrays, spots)]

        def corner_pieces(array, c):
            return [(array, (True, True, False, c)), (across(array), (True, True, True, c))]

        def own(other_core, c):
            return (False, False, other_core, c)

        sent_a, sent_b = direct(part_a), direct(part_b)
        cross_a, cross_b = across(part_a), across(part_b)
        direct_a = direct_pieces(sent_a, 0)
        far_a = corner(*sent_a)
        outs, scale = call([(part_a, own(False, 0)), (part_b, own(False, start_b)), (cross_a, own(True, 0))], None, scale)
        outs, scale = call(direct_a + [(cross_b, own(True, start_b))], outs, scale)
        far_a, scale = lax.optimization_barrier((far_a, scale))
        outs, scale = call(corner_pieces(far_a, 0), outs, scale)
        sent_b, scale = lax.optimization_barrier((sent_b, scale))
        cut = (n_block - start_b + 1) // 2 * ROW_STEP
        far_b = [corner(*(a[:cut] for a in sent_b)), corner(*(a[cut:] for a in sent_b))]
        outs, scale = call(direct_pieces(sent_b, start_b), outs, scale)
        for i, c in enumerate((start_b, start_b + cut // ROW_STEP)):
            far, scale = lax.optimization_barrier((far_b[i], scale))
            outs, scale = call(corner_pieces(far, c), outs, scale)
        return tuple(outs)

    return jax.shard_map(device_step, mesh=mesh, in_specs=(table_spec, table_spec, table_spec, P("pp", "dp", None), P("pp", "dp", None, None)), out_specs=(table_spec, table_spec, table_spec, table_spec), check_vma=False)
```

```python
import functools

import jax
import jax.numpy as jnp
from jax import lax
from jax.experimental import pallas as pl
from jax.experimental.pallas import tpu as pltpu
from jax.sharding import PartitionSpec as P


LEARN_RATE = 0.003
BETA_ONE = 0.9
BETA_TWO = 0.95
ADAM_EPS = 1e-8
WEIGHT_DECAY = 0.1
CLIP_NORM = 1.0
OPT_STEP = 10

ROW_STEP = 264
TOK_STEP = 1024
ADAMW_DEPTH = 4
ADAMW_FLOPS = 2000
VMEM_LIMIT = 60 * 1024 * 1024


def dot_nt(a, b):
    return lax.dot_general(a, b, (((1,), (1,)), ((), ())), preferred_element_type=jnp.float32)


SPREAD_CHUNKS = 24
MESH = pl.DeviceIdType.MESH


def spread_kernel(rows_valid, act_ref, ids_ref, master_ref, hid_ref, look_ref, all_ids_ref, table_ref, top_ref, sum_ref,
                  buf, hid_buf, master_buf, ids_buf, sx, sy, sz, sd, sl, so, si, load, sm, recv, recv_core, recv_ids):
    z, y, p = lax.axis_index("tp"), lax.axis_index("dp"), lax.axis_index("pp")
    x, core, odd = p // 2, p % 2, z % 2
    is_src = x == core
    x_dev = {"pp": (1 - x) * 2 + core}
    y_dev = {"dp": 1 - y}
    z_dev = {"tp": z + 1 - 2 * odd}
    core_dev = {"pp": x * 2 + 1 - core}
    plane = [{"dp": (y + dy) % 2, "pp": (p + dp) % 4} for dy in range(2) for dp in range(4) if dy + dp > 0]
    n = SPREAD_CHUNKS
    edge, main, lag, unit = n // 3, 2 * n // 3, 3, 4
    tok = act_ref.shape[0]
    size = tok // n
    rows = table_ref.shape[0]
    device = y * 4 + p
    last = len(plane)
    meet(plane + [z_dev])

    def chunk(i):
        if i < edge:
            return odd * main + i
        return i if i < main else (1 - odd) * main + (i - main)

    def span(slot, i, count=1):
        replica = y if slot == 0 else 1 - y
        return pl.ds(pl.multiple_of(replica * tok + chunk(i) * size, size), size * count)

    def remote(src, dst, send_sem, recv_sem, dev):
        pltpu.make_async_remote_copy(src_ref=src, dst_ref=dst, send_sem=send_sem, recv_sem=recv_sem, device_id=dev, device_id_type=MESH).start()

    def send(slot, i, send_sem, recv_sem, dev):
        view = buf.at[core, span(slot, i)]
        remote(view, view, send_sem, recv_sem, dev)

    def drain(sem):
        view = buf.at[0, pl.ds(0, size)]
        pltpu.make_async_copy(view, view, sem).wait()

    def arrived(slot, i):
        drain(recv.at[slot, i])

    def keep(slot, i):
        send(slot, i, sd.at[slot, i], recv_core.at[slot, i], core_dev)

    def send_ids(kind):
        pltpu.make_async_copy(ids_ref, ids_buf.at[kind, y], recv_ids.at[kind, y]).start()
        for i, dev in enumerate(plane):
            remote(ids_ref, ids_buf.at[kind, y], si.at[i], recv_ids.at[kind, y], dev)

    pl.when(p == 0)(lambda: send_ids(0))
    pl.when(p == 3)(lambda: send_ids(1))

    def master_copy(count):
        return pltpu.make_async_copy(master_ref.at[pl.ds(pl.multiple_of(device * rows, 8), count)], master_buf.at[pl.ds(0, count)], sm.at[0])

    pl.when(device < last)(lambda: master_copy(rows).start())

    @pl.when(device == last)
    def _():
        master_copy(rows_valid).start()
        if rows_valid < rows:
            master_buf[rows_valid:, :] = jnp.zeros((rows - rows_valid, master_buf.shape[1]), jnp.float32)

    @pl.when(is_src)
    def _():
        def load_copy(i):
            place = pl.ds(pl.multiple_of(chunk(i) * size, size), size)
            return pltpu.make_async_copy(act_ref.at[place], hid_buf.at[pl.ds(i * size, size)], load.at[i])

        def widen(i):
            load_copy(i).wait()
            buf[core, span(0, i), :] = hid_buf[i * size:(i + 1) * size, :].astype(jnp.float32)

        for i in range(n):
            load_copy(i).start()
        widen(0)
        for i in range(n):
            if i + 1 < n:
                widen(i + 1)
            if i < edge:
                send(0, i, sx.at[i], recv.at[0, i], x_dev)
            if i < main:
                send(0, i, sy.at[i], recv.at[1, i], y_dev)
        for i in range(n):
            keep(0, i)

    pl.when(device < last)(lambda: master_copy(rows).wait())
    pl.when(device == last)(lambda: master_copy(rows_valid).wait())
    table_ref[...] = master_buf[...].astype(jnp.bfloat16)
    valid = jnp.where(device == last, rows_valid, rows)

    def statistics(slot, i):
        place = span(slot, i, unit)
        act = buf[1, place, :].astype(jnp.bfloat16)
        hid_buf[place, :] = act
        pltpu.make_async_copy(hid_buf.at[place], hid_ref.at[place], so.at[slot, i // unit]).start()

        def tile(r, carry):
            top, total = carry
            start = pl.multiple_of(r * ROW_STEP, 8)
            logits = dot_nt(table_ref[pl.ds(start, ROW_STEP), :], act)
            row = start + lax.broadcasted_iota(jnp.int32, logits.shape, 0)
            logits = jnp.where(row < valid, logits, -jnp.inf)
            new_top = jnp.maximum(top, jnp.max(logits, axis=0, keepdims=True))
            return new_top, total * jnp.exp(top - new_top) + jnp.sum(jnp.exp(logits - new_top), axis=0, keepdims=True)

        empty = jnp.full((1, size * unit), -jnp.inf, jnp.float32)
        top, total = lax.fori_loop(0, rows // ROW_STEP, tile, (empty, jnp.zeros_like(empty)))
        where = pl.ds((y if slot == 0 else 1 - y) * (n // unit) + chunk(i) // unit, 1)
        top_ref[where, :] = top
        sum_ref[where, :] = total

    def ready(slot, i):
        drain(recv_core.at[slot, i])
        place = span(slot, i)
        pltpu.make_async_copy(buf.at[0, place], look_ref.at[place], sl.at[slot, i]).start()
        if i % unit == unit - 1:
            statistics(slot, i - unit + 1)

    def source_step(s):
        arrived(1, s)
        if s + edge < main:
            send(0, s + edge, sx.at[s + edge], recv.at[0, s + edge], x_dev)
        if s % 2 == 0:
            send(1, s, sx.at[main + s // 2], recv.at[1, s], x_dev)
        if s < edge:
            send(1, s, sz.at[1, s], recv.at[1, main + s], z_dev)
        keep(1, s)

    def other_step(s):
        if s < main:
            arrived(0, s)
            if s % 2 == 1:
                send(0, s, sy.at[s], recv.at[1, s], y_dev)
            if s < edge:
                send(0, s, sz.at[0, s], recv.at[0, main + s], z_dev)
            keep(0, s)
        i = s - edge
        if i >= 0:
            arrived(1, i)
            if i < edge:
                send(1, i, sz.at[1, i], recv.at[1, main + i], z_dev)
            keep(1, i)

    def take_far(slot, i):
        arrived(slot, i)
        keep(slot, i)

    done = set()

    def ready_once(slot, i):
        if 0 <= i and (slot, i) not in done:
            done.add((slot, i))
            ready(slot, i)

    for s in range(main + edge):
        far = main + (s - 4) // 2 if s >= 4 and s % 2 == 0 and (s - 4) // 2 < edge else None

        @pl.when(is_src)
        def _():
            if s < main:
                source_step(s)
            if far is not None:
                take_far(1, far)

        @pl.when(jnp.logical_not(is_src))
        def _():
            other_step(s)
            if far is not None:
                take_far(0, far)

        if s - lag < main:
            ready_once(0, s - lag)
        if s - edge - lag < main:
            ready_once(1, s - edge - lag)
        j = s - 4 - lag
        if j >= 0 and j % 2 == 0 and j // 2 < edge:
            ready_once(0, main + j // 2)

    @pl.when(jnp.logical_not(is_src))
    def _():
        for i in range(main, n):
            take_far(1, i)

    for slot in range(2):
        for i in range(n):
            ready_once(slot, i)

    for i in range(main):
        if i % 2 == 1:
            drain(sy.at[i])
    for i in range(edge):
        drain(sz.at[1, i])
    for slot in range(2):
        for i in range(n):
            drain(sd.at[slot, i])
            drain(sl.at[slot, i])
        for i in range(n // unit):
            view = hid_buf.at[pl.ds(0, size * unit)]
            pltpu.make_async_copy(view, view, so.at[slot, i]).wait()

    @pl.when(is_src)
    def _():
        for i in range(main + main // 2):
            drain(sx.at[i])
        for i in range(0, main, 2):
            drain(sy.at[i])

    @pl.when(jnp.logical_not(is_src))
    def _():
        for i in range(edge):
            drain(sz.at[0, i])

    for kind in range(2):
        for replica in range(2):
            pltpu.make_async_copy(ids_ref, ids_buf.at[kind, replica], recv_ids.at[kind, replica]).wait()

    @pl.when(jnp.logical_or(p == 0, p == 3))
    def _():
        for i in range(len(plane)):
            pltpu.make_async_copy(ids_ref, ids_ref, si.at[i]).wait()

    all_ids_ref[...] = ids_buf[...]


def spread_call(acts, ids, master, rows, n_repl):
    tok, dim = acts.shape
    n, unit = SPREAD_CHUNKS, 4
    ids_shape = (2, n_repl) + ids.shape
    dma = pltpu.SemaphoreType.DMA
    hbm, vmem = pl.BlockSpec(memory_space=pl.ANY), pl.BlockSpec(memory_space=pltpu.VMEM)
    stat = jax.ShapeDtypeStruct((n_repl * n // unit, tok // n * unit), jnp.float32)
    return pl.pallas_call(
        functools.partial(spread_kernel, master.shape[0] - 7 * rows),
        in_specs=[hbm, vmem, hbm],
        out_specs=[hbm, hbm, vmem, vmem, vmem, vmem],
        out_shape=[
            jax.ShapeDtypeStruct((n_repl * tok, dim), jnp.bfloat16), jax.ShapeDtypeStruct((n_repl * tok, dim), jnp.float32),
            jax.ShapeDtypeStruct(ids_shape, jnp.int32), jax.ShapeDtypeStruct((rows, dim), jnp.bfloat16), stat, stat,
        ],
        scratch_shapes=[
            pltpu.VMEM((2, n_repl * tok, dim), jnp.float32), pltpu.VMEM((n_repl * tok, dim), jnp.bfloat16), pltpu.VMEM((rows, dim), jnp.float32),
            pltpu.VMEM(ids_shape, jnp.int32),
            dma((n + n // 2,)), dma((n,)), dma((2, n // 3)), dma((2, n)), dma((2, n)), dma((2, n // unit)), dma((8,)),
            dma((n,)), dma((1,)), dma((2, n)), dma((2, n)), dma((2, 2)),
        ],
        compiler_params=pltpu.CompilerParams(collective_id=0, has_side_effects=True, vmem_limit_bytes=VMEM_LIMIT),
        name="spread",
    )(acts, ids, master)


def slice_partners(z, y, p):
    return [
        {"pp": (p // 2) * 2 + 1 - p % 2}, {"pp": (1 - p // 2) * 2 + p % 2}, {"dp": 1 - y},
        {"tp": z + 1 - 2 * (z % 2)}, {"tp": (z + 2) % 4},
    ]


def meet(partners):
    barrier = pltpu.get_barrier_semaphore()
    for dev in partners:
        pl.semaphore_signal(barrier, inc=1, device_id=dev, device_id_type=MESH)
    pl.semaphore_wait(barrier, len(partners))


def combine_kernel(scale, in_ref, top_ref, inv_ref, mine, theirs, send_sem, recv_sem):
    z, y, p = lax.axis_index("tp"), lax.axis_index("dp"), lax.axis_index("pp")
    partners = slice_partners(z, y, p)
    meet(partners)
    half = in_ref.shape[0] // 2
    mine[0] = in_ref[...]
    for step, dev in enumerate(partners):
        copy = pltpu.make_async_remote_copy(src_ref=mine.at[step], dst_ref=theirs.at[step], send_sem=send_sem.at[step], recv_sem=recv_sem.at[step], device_id=dev, device_id_type=MESH)
        copy.start()
        copy.wait()
        top_a, sum_a = mine[step, :half], mine[step, half:]
        top_b, sum_b = theirs[step, :half], theirs[step, half:]
        top = jnp.maximum(top_a, top_b)
        total = sum_a * jnp.exp(top_a - top) + sum_b * jnp.exp(top_b - top)
        if step + 1 < len(partners):
            mine[step + 1, :half] = top
            mine[step + 1, half:] = total
        else:
            top_ref[...] = top
            inv_ref[...] = 1.0 / (total * scale)


def combine_call(local, scale):
    rows, lanes = local.shape
    shape = jax.ShapeDtypeStruct((rows // 2, lanes), jnp.float32)
    return pl.pallas_call(
        functools.partial(combine_kernel, scale),
        in_specs=[pl.BlockSpec(memory_space=pltpu.VMEM)],
        out_specs=[pl.BlockSpec(memory_space=pltpu.VMEM)] * 2,
        out_shape=[shape, shape],
        scratch_shapes=[pltpu.VMEM((5, rows, lanes), jnp.float32), pltpu.VMEM((5, rows, lanes), jnp.float32), pltpu.SemaphoreType.DMA((5,)), pltpu.SemaphoreType.DMA((5,))],
        compiler_params=pltpu.CompilerParams(collective_id=1, has_side_effects=True),
        name="combine",
    )(local)


def norm_kernel(n_dev, *refs):
    *in_refs, out_ref, mine, theirs, send_sem, recv_sem = refs
    z, y, p = lax.axis_index("tp"), lax.axis_index("dp"), lax.axis_index("pp")
    n_tp, n_repl, n_stage = n_dev
    steps = [(a, b, c) for a in range(n_tp) for b in range(n_repl) for c in range(n_stage)][1:]
    devices = [{"tp": (z + a) % n_tp, "dp": (y + b) % n_repl, "pp": (p + c) % n_stage} for a, b, c in steps]
    meet(devices)
    mine[...] = jnp.full(mine.shape, jnp.sum(sum(ref[...] for ref in in_refs)))
    me = (z * n_repl + y) * n_stage + p
    copies = []
    for i, dev in enumerate(devices):
        copy = pltpu.make_async_remote_copy(src_ref=mine, dst_ref=theirs.at[me], send_sem=send_sem.at[i], recv_sem=recv_sem.at[me], device_id=dev, device_id_type=MESH)
        copy.start()
        copies.append(copy)
    own = pltpu.make_async_copy(mine, theirs.at[me], recv_sem.at[me])
    own.start()
    for i in range(len(steps) + 1):
        pltpu.make_async_copy(mine, theirs.at[i], recv_sem.at[i]).wait()
    for copy in copies:
        copy.wait_send()
    total = jnp.sum(theirs[...], axis=0)
    out_ref[...] = CLIP_NORM / jnp.maximum(jnp.sqrt(total), CLIP_NORM)


def norm_call(squares, n_dev):
    n_all = n_dev[0] * n_dev[1] * n_dev[2]
    vmem = pl.BlockSpec(memory_space=pltpu.VMEM)
    return pl.pallas_call(
        functools.partial(norm_kernel, n_dev),
        in_specs=[vmem] * len(squares),
        out_specs=vmem,
        out_shape=jax.ShapeDtypeStruct((8, 128), jnp.float32),
        scratch_shapes=[pltpu.VMEM((8, 128), jnp.float32), pltpu.VMEM((n_all, 8, 128), jnp.float32), pltpu.SemaphoreType.DMA((n_all,)), pltpu.SemaphoreType.DMA((n_all,))],
        compiler_params=pltpu.CompilerParams(collective_id=2, has_side_effects=True),
        name="norm",
    )(*squares)


def grad_kernel(offset, tok_count, scal_ref, table_ref, hid_ref, dx_ref, max_ref, inv_ref, lab_ref, ids_ref, *out_refs):
    *grad_refs, sq_ref = out_refs
    step = pl.program_id(0)
    rows = grad_refs[0].shape[0]

    @pl.when(step == 0)
    def _():
        for grad_ref in grad_refs:
            grad_ref[...] = jnp.zeros_like(grad_ref)

    hid = hid_ref[...]
    look = dx_ref[...].astype(jnp.bfloat16)
    for start in range(0, rows * len(grad_refs), ROW_STEP):
        logits = dot_nt(table_ref[start:start + ROW_STEP, :], hid)
        local = offset + start + lax.broadcasted_iota(jnp.int32, logits.shape, 0)
        row = jnp.where(local < scal_ref[1], local + scal_ref[0], -1)
        prob = jnp.where(local < scal_ref[1], jnp.exp(logits - max_ref[...]) * inv_ref[...], 0.0)
        dlog = (prob - jnp.where(row == lab_ref[...], 1.0 / tok_count, 0.0)).astype(jnp.bfloat16)
        hot = jnp.where(row == ids_ref[...], 1.0, 0.0).astype(jnp.bfloat16)
        part = jnp.dot(dlog, hid, preferred_element_type=jnp.float32)
        part += jnp.dot(hot, look, preferred_element_type=jnp.float32)
        grad_refs[start // rows][start % rows:start % rows + ROW_STEP, :] += part

    @pl.when(step == pl.num_programs(0) - 1)
    def _():
        square = jnp.zeros_like(sq_ref)
        for grad_ref in grad_refs:
            grad = grad_ref[...] * 0.5
            grad_ref[...] = grad
            square += jnp.sum(grad * grad, axis=0, keepdims=True)
        sq_ref[...] = square


def grad_call(scal, table_bf, hid, dx, top, inv, labels, ids, offset, tok_count):
    tokens, dim = hid.shape
    rows, n_out = table_bf.shape[0] // 2, 1
    half = offset // rows
    tok_spec = pl.BlockSpec((1, TOK_STEP), lambda t: (0, t))
    act_spec = pl.BlockSpec((TOK_STEP, dim), lambda t: (t, 0))
    return pl.pallas_call(
        functools.partial(grad_kernel, offset, tok_count),
        grid=(tokens // TOK_STEP,),
        in_specs=[
            pl.BlockSpec(memory_space=pltpu.SMEM),
            pl.BlockSpec((rows * n_out, dim), lambda t: (half, 0)),
            act_spec, act_spec, tok_spec, tok_spec, tok_spec, tok_spec,
        ],
        out_specs=[pl.BlockSpec((rows, dim), lambda t: (0, 0))] * n_out + [pl.BlockSpec((1, dim), lambda t: (0, 0))],
        out_shape=[jax.ShapeDtypeStruct((rows, dim), jnp.float32)] * n_out + [jax.ShapeDtypeStruct((1, dim), jnp.float32)],
        compiler_params=pltpu.CompilerParams(vmem_limit_bytes=VMEM_LIMIT),
        cost_estimate=pl.CostEstimate(flops=6 * tokens * rows * n_out * dim, bytes_accessed=6 * tokens * dim, transcendentals=tokens * rows * n_out),
    )(scal, table_bf, hid, dx, top, inv, labels, ids)


def adamw_kernel(counts, spots, n_alias, *refs):
    n_piece = len(counts)
    scale_ref = refs[0]
    state_refs = refs[1:4]
    piece_refs = refs[4:4 + n_piece]
    *out_refs, out_scale, in_buf, out_buf, bf_buf, in_sem, out_sem = refs[4 + n_piece + n_alias:]
    y, p = lax.axis_index("dp"), lax.axis_index("pp")
    x, core = p // 2, p % 2
    out_scale[...] = scale_ref[...]
    scale = scale_ref[0:1, 0:1]
    vocab = state_refs[0].shape[0]
    depth, short, sub_rows = in_buf.shape[0], vocab % ROW_STEP, 24
    blocks = [(j, i) for j, count in enumerate(counts) for i in range(count)]

    def by_length(row, action):
        if short == 0:
            action(ROW_STEP)
        else:
            pl.when(row + ROW_STEP <= vocab)(lambda: action(ROW_STEP))
            pl.when(row + ROW_STEP > vocab)(lambda: action(short))

    def first_row(b):
        j, i = blocks[b]
        flip_y, flip_x, flip_core, block = spots[j]
        yy, xx, cc = (1 - v if flip else v for v, flip in ((y, flip_y), (x, flip_x), (core, flip_core)))
        own_blocks = -(-vocab // (8 * ROW_STEP))
        return pl.multiple_of(((yy * 4 + xx * 2 + cc) * own_blocks + block + i) * ROW_STEP, 8)

    def grad_copy(b):
        j, i = blocks[b]
        return pltpu.make_async_copy(piece_refs[j].at[pl.ds(i * ROW_STEP, ROW_STEP)], in_buf.at[b % depth, 3], in_sem.at[b % depth, 3])

    def in_copies(b, row, size):
        slot = b % depth
        return [pltpu.make_async_copy(ref.at[pl.ds(row, size)], in_buf.at[slot, k, pl.ds(0, size)], in_sem.at[slot, k]) for k, ref in enumerate(state_refs)]

    def out_copies(b, row, size):
        slot = b % depth
        sources = [out_buf.at[slot, k] for k in range(3)] + [bf_buf.at[slot]]
        return [pltpu.make_async_copy(src.at[pl.ds(0, size)], ref.at[pl.ds(row, size)], out_sem.at[slot, k]) for k, (src, ref) in enumerate(zip(sources, out_refs))]

    def each(make, b, method):
        row = first_row(b)

        def act(size):
            for copy in make(b, row, size):
                getattr(copy, method)()

        by_length(row, act)

    def start_in(b):
        each(in_copies, b, "start")
        grad_copy(b).start()

    for b in range(min(depth - 1, len(blocks))):
        start_in(b)
    for b in range(len(blocks)):
        if b + depth - 1 < len(blocks):
            start_in(b + depth - 1)
        each(in_copies, b, "wait")
        grad_copy(b).wait()
        if b >= depth:
            each(out_copies, b - depth, "wait")
        slot = b % depth

        def body(i, carry):
            rows = pl.ds(pl.multiple_of(i * sub_rows, 8), sub_rows)
            grad = in_buf[slot, 3, rows, :] * scale
            avg = BETA_ONE * in_buf[slot, 1, rows, :] + (1.0 - BETA_ONE) * grad
            sq = BETA_TWO * in_buf[slot, 2, rows, :] + (1.0 - BETA_TWO) * grad * grad
            step_dir = (avg / (1.0 - BETA_ONE ** OPT_STEP)) / (jnp.sqrt(sq / (1.0 - BETA_TWO ** OPT_STEP)) + ADAM_EPS)
            old = in_buf[slot, 0, rows, :]
            new = old - LEARN_RATE * (step_dir + WEIGHT_DECAY * old)
            out_buf[slot, 0, rows, :] = new
            out_buf[slot, 1, rows, :] = avg
            out_buf[slot, 2, rows, :] = sq
            bf_buf[slot, rows, :] = new.astype(jnp.bfloat16)
            return carry

        lax.fori_loop(0, ROW_STEP // sub_rows, body, 0)
        each(out_copies, b, "start")
    for b in range(max(0, len(blocks) - depth), len(blocks)):
        each(out_copies, b, "wait")


def adamw_call(scale, state, pieces, spots, outs):
    vocab, dim = state[0].shape
    counts = tuple(p.shape[0] // ROW_STEP for p in pieces)
    extra = list(outs) if outs is not None else []
    n_in = 1 + 3 + len(pieces)
    shapes = [jax.ShapeDtypeStruct((vocab, dim), jnp.float32)] * 3 + [jax.ShapeDtypeStruct((vocab, dim), jnp.bfloat16)]
    n_el = sum(counts) * ROW_STEP * dim
    hbm, vmem = pl.BlockSpec(memory_space=pl.ANY), pl.BlockSpec(memory_space=pltpu.VMEM)
    return pl.pallas_call(
        functools.partial(adamw_kernel, counts, spots, len(extra)),
        in_specs=[vmem] + [hbm] * (3 + len(pieces) + len(extra)),
        out_specs=[hbm] * 4 + [vmem],
        out_shape=shapes + [jax.ShapeDtypeStruct((8, 128), jnp.float32)],
        scratch_shapes=[
            pltpu.VMEM((ADAMW_DEPTH, 4, ROW_STEP, dim), jnp.float32), pltpu.VMEM((ADAMW_DEPTH, 3, ROW_STEP, dim), jnp.float32),
            pltpu.VMEM((ADAMW_DEPTH, ROW_STEP, dim), jnp.bfloat16), pltpu.SemaphoreType.DMA((ADAMW_DEPTH, 4)), pltpu.SemaphoreType.DMA((ADAMW_DEPTH, 4)),
        ],
        input_output_aliases={n_in + i: i for i in range(len(extra))},
        compiler_params=pltpu.CompilerParams(vmem_limit_bytes=VMEM_LIMIT),
        cost_estimate=pl.CostEstimate(flops=ADAMW_FLOPS * n_el, bytes_accessed=30 * n_el, transcendentals=n_el),
    )(scale, *state, *pieces, *extra)


def solution(mesh):
    n_stage, n_repl, n_tp = mesh.shape["pp"], mesh.shape["dp"], mesh.shape["tp"]
    n_plane = n_stage * n_repl
    table_spec = P("tp", None)
    axes = ("tp", "dp", "pp")
    x_swap = [(i, i ^ 2) for i in range(n_stage)]
    core_swap = [(i, i ^ 1) for i in range(n_stage)]
    y_swap = [(0, 1), (1, 0)]
    corner_pairs = [(yy * n_stage + q, (1 - yy) * n_stage + q if q % 2 == 0 else yy * n_stage + (q ^ 2)) for yy in range(n_repl) for q in range(n_stage)]

    def device_step(master, exp_avg, exp_avg_sq, stage_ids, stage_acts):
        z, y, p = (lax.axis_index(a) for a in axes)
        vocab, dim = master.shape
        tok = stage_ids.shape[1] * stage_ids.shape[2]
        own_rows = -(-vocab // (n_plane * 6 * ROW_STEP)) * 6 * ROW_STEP
        plane = y * n_stage + p

        first_row = plane * own_rows
        valid = jnp.minimum(own_rows, vocab - first_row)
        scal = jnp.stack([z * vocab + first_row, valid]).astype(jnp.int32)

        acts = stage_acts.reshape(tok, dim)
        hid_bf, dx, all_ids, table_bf, top_own, sum_own = spread_call(acts, stage_ids.reshape(tok // 128, 128), master, own_rows, n_repl)
        ids, labels = all_ids[0].reshape(1, -1), all_ids[1].reshape(1, -1)
        rows_a = own_rows // (2 * ROW_STEP) * ROW_STEP
        local = jnp.concatenate([top_own.reshape(-1, 128), sum_own.reshape(-1, 128)], axis=0)
        top, inv = (a.reshape(1, -1) for a in combine_call(local, float(tok)))

        n_block = own_rows // ROW_STEP
        start_b = rows_a // ROW_STEP
        part_a, sq_a = grad_call(scal, table_bf, hid_bf, dx, top, inv, labels, ids, 0, tok)
        part_b, sq_b = grad_call(scal, table_bf, hid_bf, dx, top, inv, labels, ids, rows_a, tok)
        scale = norm_call([sq_a, sq_b], (n_tp, n_repl, n_stage))
        part_b, scale = lax.optimization_barrier((part_b, scale))

        def across(a):
            return lax.ppermute(a, "pp", core_swap)

        def direct(a):
            from_x = lax.ppermute(a, "pp", x_swap)
            return from_x, lax.ppermute(a, "dp", y_swap)

        def corner(from_x, from_y):
            payload = jnp.where(p % 2 == 0, from_x, from_y)
            return lax.ppermute(payload, ("dp", "pp"), corner_pairs)

        def call(pieces, outs, scale):
            *outs, scale = adamw_call(scale, (master, exp_avg, exp_avg_sq), [a for a, _ in pieces], tuple(spot for _, spot in pieces), outs)
            return outs, scale

        def direct_pieces(arrays, c):
            spots = ((False, True), (True, False))
            return [(a, (*spot, False, c)) for a, spot in zip(arrays, spots)] + [(across(a), (*spot, True, c)) for a, spot in zip(arrays, spots)]

        def corner_pieces(array, c):
            return [(array, (True, True, False, c)), (across(array), (True, True, True, c))]

        def own(other_core, c):
            return (False, False, other_core, c)

        sent_a, sent_b = direct(part_a), direct(part_b)
        cross_a, cross_b = across(part_a), across(part_b)
        direct_a = direct_pieces(sent_a, 0)
        far_a = corner(*sent_a)
        outs, scale = call([(part_a, own(False, 0)), (part_b, own(False, start_b)), (cross_a, own(True, 0))], None, scale)
        outs, scale = call(direct_a + [(cross_b, own(True, start_b))], outs, scale)
        far_a, scale = lax.optimization_barrier((far_a, scale))
        outs, scale = call(corner_pieces(far_a, 0), outs, scale)
        sent_b, scale = lax.optimization_barrier((sent_b, scale))
        cut = (n_block - start_b + 1) // 2 * ROW_STEP
        far_b = [corner(*(a[:cut] for a in sent_b)), corner(*(a[cut:] for a in sent_b))]
        outs, scale = call(direct_pieces(sent_b, start_b), outs, scale)
        for i, c in enumerate((start_b, start_b + cut // ROW_STEP)):
            far, scale = lax.optimization_barrier((far_b[i], scale))
            outs, scale = call(corner_pieces(far, c), outs, scale)
        return tuple(outs)

    return jax.shard_map(device_step, mesh=mesh, in_specs=(table_spec, table_spec, table_spec, P("pp", "dp", None), P("pp", "dp", None, None)), out_specs=(table_spec, table_spec, table_spec, table_spec), check_vma=False)
```
